128 devices in a mesh: row: 16 (over z_lo, x, core), col: 8 (over z_hi, y).
Axes of the slice: x: 4, y: 4, z: 4 (z_hi: 2, z_lo: 2; z = z_hi * 2 + z_lo), core: 2. Of those that a mesh axis runs over, the one named last changes fastest.
Arguments:
- gate_weight: bfloat16 [4096, 14336], P('row', 'col'), may hold values from -6 to 6
- up_weight: bfloat16 [4096, 14336], P('row', 'col'), may hold values from -6 to 6
- down_weight: bfloat16 [14336, 4096], P('row', 'col'), may hold values from -6 to 6
- gate_row_bits: int32 [4096], P('row'), may hold values from 0 to 1
- gate_col_bits: int32 [14336], P('col'), may hold values from 0 to 1
- up_row_bits: int32 [4096], P('row'), may hold values from 0 to 1
- up_col_bits: int32 [14336], P('col'), may hold values from 0 to 1
- down_row_bits: int32 [14336], P('row'), may hold values from 0 to 1
- down_col_bits: int32 [4096], P('col'), may hold values from 0 to 1
- block_order: int32 [7], replicated, may hold values from 0 to 6, each once
Outputs:
- gate_out: bfloat16 [4096, 14336], P('row', 'col')
- up_out: bfloat16 [4096, 14336], P('row', 'col')
- down_out: bfloat16 [14336, 4096], P('row', 'col')
The draws below stay inside these ranges and needn't reach their ends.
Inputs may be any that keep to these rules, and one draw needn't show every extreme that they name: block_order is a permutation of the 7 block numbers.
All inputs are finite; a program needn't handle non-finite values.
Results may differ from the reference program's by a relative error of at most 0.0013.
Values sent between devices are 32-bit elements; how exact they have to be, the bound alone decides.
A program may use at most 64 MiB of HBM per device.

```python
import jax
import jax.numpy as jnp
from jax import lax

D = 4096
FF = 14336
BLK = 128
GROUPS = 16
HBLOCKS = 7


def touch_ends(values, rng, low, high):
    dims = values.shape
    spot = [jax.random.randint(jax.random.fold_in(rng, axis), (), 0, dims[axis]) for axis in range(len(dims))]
    values = values.at[tuple(spot)].set(low)
    longest = dims.index(max(dims))
    spot[longest] = (spot[longest] + 1) % dims[longest]
    return values.at[tuple(spot)].set(high)


def block_scale(key, extent, split, smallest, largest):
    loudness = 1.0
    for axis_at, blocks in split:
        draws = jax.random.uniform(jax.random.fold_in(jax.random.fold_in(key, 6), axis_at), (blocks,), jnp.float32, smallest / len(split), largest / len(split))
        loudness = loudness * jnp.repeat(jnp.exp(draws), extent[axis_at] // blocks).reshape((-1,) + (1,) * (len(extent) - 1 - axis_at))
    return loudness


def normal_values(key, extent, scale, limit, shards=(), dtype=jnp.bfloat16):
    array = scale * jax.random.normal(key, extent, jnp.float32)
    if shards:
        array = array * block_scale(key, extent, shards, -0.22, 0.18)
    return jnp.clip(array, -limit, limit).astype(dtype)


def setup_inputs(seed: int = 0) -> dict:
    splits = jax.random.split(jax.random.key(seed), 11)
    return {
        "gate_weight": normal_values(splits[0], (D, FF), 1.0, 6.0, ((0, 16), (1, 8))),
        "up_weight": normal_values(splits[1], (D, FF), 1.0, 6.0, ((0, 16), (1, 8))),
        "down_weight": normal_values(splits[2], (FF, D), 1.0, 6.0, ((0, 16), (1, 8))),
        "gate_row_bits": touch_ends(jax.random.randint(splits[3], (D,), 0, 2), jax.random.fold_in(splits[3], 1), 0, 1).astype(jnp.int32),
        "gate_col_bits": touch_ends(jax.random.randint(splits[4], (FF,), 0, 2), jax.random.fold_in(splits[4], 1), 0, 1).astype(jnp.int32),
        "up_row_bits": touch_ends(jax.random.randint(splits[5], (D,), 0, 2), jax.random.fold_in(splits[5], 1), 0, 1).astype(jnp.int32),
        "up_col_bits": touch_ends(jax.random.randint(splits[6], (FF,), 0, 2), jax.random.fold_in(splits[6], 1), 0, 1).astype(jnp.int32),
        "down_row_bits": touch_ends(jax.random.randint(splits[7], (FF,), 0, 2), jax.random.fold_in(splits[7], 1), 0, 1).astype(jnp.int32),
        "down_col_bits": touch_ends(jax.random.randint(splits[8], (D,), 0, 2), jax.random.fold_in(splits[8], 1), 0, 1).astype(jnp.int32),
        "block_order": jax.random.permutation(splits[9], HBLOCKS).astype(jnp.int32),
    }


HIGHEST = lax.Precision.HIGHEST


def sylvester(order_size):
    indices = lax.iota(jnp.int32, order_size)
    both = jnp.bitwise_and(indices[:, None], indices[None, :])
    folded = jnp.zeros_like(both)
    for shift in range(max(order_size.bit_length() - 1, 1)):
        folded = jnp.bitwise_xor(folded, jnp.right_shift(both, shift))
    parity = jnp.bitwise_and(folded, 1)
    return (1 - 2 * parity).astype(jnp.float32)


def split_sizes(order_size):
    exponent = order_size.bit_length() - 1
    leading = 1 << (exponent // 2)
    return leading, order_size // leading


def mix_model_rows(matrix):
    leading, trailing = split_sizes(matrix.shape[0])
    shaped = matrix.reshape(leading, trailing, matrix.shape[1])
    shaped = jnp.einsum('ab,bcm->acm', sylvester(leading), shaped, precision=HIGHEST)
    shaped = jnp.einsum('cd,adm->acm', sylvester(trailing), shaped, precision=HIGHEST)
    return shaped.reshape(matrix.shape)


def mix_model_cols(matrix):
    leading, trailing = split_sizes(matrix.shape[1])
    shaped = matrix.reshape(matrix.shape[0], leading, trailing)
    shaped = jnp.einsum('ab,mbc->mac', sylvester(leading), shaped, precision=HIGHEST)
    shaped = jnp.einsum('cd,mad->mac', sylvester(trailing), shaped, precision=HIGHEST)
    return shaped.reshape(matrix.shape)


def mix_hidden_cols(matrix, block_order):
    shaped = matrix.reshape(matrix.shape[0], GROUPS, HBLOCKS, BLK)
    shaped = jnp.einsum('gk,mkhb->mghb', sylvester(GROUPS), shaped, precision=HIGHEST)
    shaped = jnp.einsum('bc,mghc->mghb', sylvester(BLK), shaped, precision=HIGHEST)
    shaped = jnp.take(shaped, block_order, axis=2)
    return shaped.reshape(matrix.shape)


def mix_hidden_rows(matrix, block_order):
    shaped = matrix.reshape(GROUPS, HBLOCKS, BLK, matrix.shape[1])
    shaped = jnp.einsum('gk,khbm->ghbm', sylvester(GROUPS), shaped, precision=HIGHEST)
    shaped = jnp.einsum('bc,ghcm->ghbm', sylvester(BLK), shaped, precision=HIGHEST)
    shaped = jnp.take(shaped, block_order, axis=1)
    return shaped.reshape(matrix.shape)


def sign_values(sign_bits):
    return (1 - 2 * sign_bits).astype(jnp.float32)


def reference(gate_weight, up_weight, down_weight, gate_row_bits, gate_col_bits, up_row_bits, up_col_bits, down_row_bits, down_col_bits, block_order):
    factor = (D * GROUPS * BLK) ** -0.5

    def transform_in(weight, row_bits, col_bits):
        signed = weight.astype(jnp.float32) * sign_values(row_bits)[:, None] * sign_values(col_bits)[None, :]
        mixed = mix_hidden_cols(mix_model_rows(signed), block_order)
        return (mixed * factor).astype(jnp.bfloat16)

    signed = down_weight.astype(jnp.float32) * sign_values(down_row_bits)[:, None] * sign_values(down_col_bits)[None, :]
    mixed = mix_hidden_rows(mix_model_cols(signed), block_order)
    down_out = (mixed * factor).astype(jnp.bfloat16)
    gate_out = transform_in(gate_weight, gate_row_bits, gate_col_bits)
    up_out = transform_in(up_weight, up_row_bits, up_col_bits)
    return gate_out, up_out, down_out
```

```python
import jax
import jax.numpy as jnp
from jax import lax
from jax.experimental import pallas as pl
from jax.experimental.pallas import tpu as pltpu
from jax.sharding import PartitionSpec as P

D = 4096
BLK = 128
GROUPS = 16
HBLOCKS = 7
FACTOR = (D * GROUPS * BLK) ** (-0.5)
MESH = pl.DeviceIdType.MESH
LANES = 6
SLOTS = 6
CHUNK = (128, 256)
CORE_AFTER = (1, 3, 1, 3, 1, 3)
VMEM_LIMIT = 55 * 1024 * 1024


def sylvester(order_size):
    rows = lax.broadcasted_iota(jnp.int32, (order_size, order_size), 0)
    both = jnp.bitwise_and(rows, lax.broadcasted_iota(jnp.int32, rows.shape, 1))
    for shift in (4, 2, 1):
        both = jnp.bitwise_xor(both, jnp.right_shift(both, shift))
    return (1 - 2 * jnp.bitwise_and(both, 1)).astype(jnp.float32)


def signs_of(bits):
    return (1 - 2 * bits).astype(jnp.float32)


def split(values):
    high = values.astype(jnp.bfloat16)
    return high, (values - high.astype(jnp.float32)).astype(jnp.bfloat16)


def dot(left, right):
    return jnp.dot(left, right, preferred_element_type=jnp.float32)


def dot_nt(left, right):
    return lax.dot_general(
        left, right, (((1,), (1,)), ((), ())), preferred_element_type=jnp.float32
    )


def kernel(
    order_ref,
    gate_row,
    gate_col,
    up_row,
    up_col,
    down_row,
    down_col,
    gate_hbm,
    up_hbm,
    down_hbm,
    gate_out,
    up_out,
    down_out,
    own,
    got0,
    got1,
    got2,
    got3,
    got4,
    got5,
    got_core,
    sent,
    gate_in,
    up_in,
    down_in,
    plain,
    gate_left,
    up_left,
    down_right,
    in_sem,
    send_sem,
    recv_sem,
    core_send_sem,
    core_recv_sem,
):
    got = (got0, got1, got2, got3, got4, got5)
    row, col = lax.axis_index("row"), lax.axis_index("col")
    core = lax.rem(row, 2)
    x = lax.rem(lax.div(row, 2), 4)
    z_lo = lax.div(row, 8)
    y = lax.rem(col, 4)
    z_hi = lax.div(col, 4)

    def flip(bit):
        return 1 - bit

    def place(z_lo, x, core, z_hi, y):
        return (z_lo * 8 + x * 2 + core, z_hi * 4 + y)

    def one(v):
        return v + 1 - 2 * lax.rem(v, 2)

    partners = (
        (place(z_lo, one(x), core, z_hi, y), place(z_lo, 3 - x, core, z_hi, y)),
        (place(z_lo, x, core, z_hi, one(y)), place(z_lo, x, core, z_hi, 3 - y)),
        (place(flip(z_lo), x, core, z_hi, y), place(flip(z_lo), x, core, flip(z_hi), y)),
    )
    core_partner = place(z_lo, x, flip(core), z_hi, y)

    def as_sign(bit):
        return (1 - 2 * bit).astype(jnp.float32)

    low = (as_sign(lax.rem(x, 2)), as_sign(lax.rem(y, 2)), as_sign(z_lo))
    high = (as_sign(lax.div(x, 2)), as_sign(lax.div(y, 2)), as_sign(z_hi))
    core_sign = as_sign(core)

    def axis_of(group, slot):
        return (group // 2 + slot // 2) % 3

    def partner(group, slot):
        return partners[axis_of(group, slot)][(slot + group) % 2]

    def source(group, slot):
        if slot == 0:
            return own
        if slot % 2 == 1:
            return sent
        return got_core if CORE_AFTER[group] == slot - 1 else got[slot - 1]

    def copy(group, slot, chunk):
        return pltpu.make_async_remote_copy(
            src_ref=source(group, slot).at[group, chunk],
            dst_ref=got[slot].at[group, chunk],
            send_sem=send_sem.at[slot, group, chunk],
            recv_sem=recv_sem.at[slot, group, chunk],
            device_id=partner(group, slot),
            device_id_type=MESH,
        )

    def core_copy(group, chunk):
        return pltpu.make_async_remote_copy(
            src_ref=got[CORE_AFTER[group]].at[group, chunk],
            dst_ref=got_core.at[group, chunk],
            send_sem=core_send_sem.at[group, chunk],
            recv_sem=core_recv_sem.at[group, chunk],
            device_id=core_partner,
            device_id_type=MESH,
        )

    loads = (
        pltpu.make_async_copy(gate_hbm, gate_in, in_sem.at[0]),
        pltpu.make_async_copy(up_hbm, up_in, in_sem.at[1]),
        pltpu.make_async_copy(down_hbm, down_in, in_sem.at[2]),
    )
    for load in loads:
        load.start()

    barrier = pltpu.get_barrier_semaphore()
    for pair in partners:
        for device in pair:
            pl.semaphore_signal(barrier, inc=1, device_id=device, device_id_type=MESH)
    pl.semaphore_signal(barrier, inc=1, device_id=core_partner, device_id_type=MESH)

    hadamard = sylvester(2 * BLK)
    plain[...] = hadamard.astype(jnp.bfloat16)
    gate_left[...] = (hadamard * signs_of(gate_row[...])).astype(jnp.bfloat16)
    up_left[...] = (hadamard * signs_of(up_row[...])).astype(jnp.bfloat16)
    for half in range(2):
        down_right[half] = (
            hadamard * signs_of(down_col[:, half * 256 : (half + 1) * 256])
        ).astype(jnp.bfloat16)

    def pick(block, pieces):
        chosen = pieces(0)
        for other in range(1, HBLOCKS):
            chosen = jnp.where(block == other, pieces(other), chosen)
        return chosen

    def mix_in(weights, left, col_bits, group, chunk):
        block = order_ref[chunk]

        def both(ref, index):
            return jnp.concatenate([ref(index), ref(index + HBLOCKS)], axis=1)

        pair = pick(block, lambda k: both(lambda i: weights[:, i * BLK : (i + 1) * BLK], k))
        bits = pick(block, lambda k: both(lambda i: col_bits[i : i + 1, :], k))
        upper, lower = split(dot(left[...], pair) * signs_of(bits))
        mixed = dot(upper, plain[...]) + dot(lower, plain[...])
        own[group, chunk] = mixed[:BLK]
        own[group + 1, chunk] = mixed[BLK:]

    def mix_down(chunk):
        block = order_ref[chunk]
        weights = pick(block, lambda k: down_in[k * BLK : (k + 1) * BLK, :])
        bits = pick(block, lambda k: down_row[k : k + 1, :])
        first = dot_nt(weights[:, :256], down_right[0])
        second = dot_nt(weights[:, 256:], down_right[1])
        left = (plain[:BLK, :BLK].astype(jnp.float32) * signs_of(bits)).astype(jnp.bfloat16)
        for group, values in ((4, first + second), (5, first - second)):
            upper, lower = split(values)
            own[group, chunk] = dot(left, upper) + dot(left, lower)

    loads[0].wait()
    loads[1].wait()
    loads[2].wait()

    def spread(chunk, carry):
        mix_in(gate_in, gate_left, gate_col, 0, chunk)

        @pl.when(chunk == 0)
        def _():
            pl.semaphore_wait(barrier, 7)

        @pl.when(chunk > 0)
        def _():
            copy(4, 0, chunk - 1).start()
            copy(5, 0, chunk - 1).start()

        mix_in(up_in, up_left, up_col, 2, chunk)
        copy(0, 0, chunk).start()
        copy(1, 0, chunk).start()
        mix_down(chunk)
        copy(2, 0, chunk).start()
        copy(3, 0, chunk).start()
        return carry

    lax.fori_loop(0, HBLOCKS, spread, 0)
    copy(4, 0, HBLOCKS - 1).start()
    copy(5, 0, HBLOCKS - 1).start()

    def first_half(slot):
        def step(chunk, carry):
            for group in range(LANES):
                axis = axis_of(group, slot)
                q = low[axis] if group % 2 == 0 else low[axis] * high[axis]
                if slot > 0:
                    copy(group, slot - 1, chunk).wait_send()
                copy(group, slot, chunk).wait_recv()
                mine = source(group, slot)[group, chunk]
                theirs = q * got[slot][group, chunk]
                got[slot][group, chunk] = mine + theirs
                sent[group, chunk] = mine - theirs
                if group > 0:
                    copy(group - 1, slot + 1, chunk).start()
            copy(LANES - 1, slot + 1, chunk).start()
            return carry

        lax.fori_loop(0, HBLOCKS, step, 0)

    def combined(group, slot, chunk, scale):
        axis = axis_of(group, slot)
        fk = low[axis] * high[axis] * scale
        fr = scale if group % 2 == 0 else high[axis] * scale
        return fr * got[slot][group, chunk] + fk * got[slot - 1][group, chunk]

    def second_half(slot):
        with_core = [group for group in range(LANES) if CORE_AFTER[group] == slot]

        def step(chunk, carry):
            @pl.when(chunk < HBLOCKS)
            def _():
                ready = None
                for group in range(LANES):
                    copy(group, slot - 1, chunk).wait_send()
                    copy(group, slot, chunk).wait_recv()
                    got[slot][group, chunk] = combined(group, slot, chunk, 1.0)
                    if ready is not None:
                        ready.start()
                    if group in with_core:
                        ready = core_copy(group, chunk)
                    else:
                        ready = copy(group, slot + 1, chunk)
                ready.start()

            @pl.when(chunk > 0)
            def _():
                last = chunk - 1
                ready = None
                for group in with_core:
                    core_copy(group, last).wait_recv()
                    got_core[group, last] = (
                        got_core[group, last] + core_sign * got[slot][group, last]
                    )
                    core_copy(group, last).wait_send()
                    if ready is not None:
                        ready.start()
                    ready = copy(group, slot + 1, last)
                ready.start()

            return carry

        lax.fori_loop(0, HBLOCKS + 1, step, 0)

    def finish(slot):
        def step(chunk, carry):
            first = pl.ds(pl.multiple_of(chunk * BLK, BLK), BLK)
            second = pl.ds(pl.multiple_of((chunk + HBLOCKS) * BLK, BLK), BLK)
            for group in range(LANES):
                copy(group, slot - 1, chunk).wait_send()
                copy(group, slot, chunk).wait_recv()
                copy(group, slot, chunk).wait_send()
                values = combined(group, slot, chunk, FACTOR).astype(jnp.bfloat16)
                half = group % 2
                if group < 4:
                    out = gate_out if group < 2 else up_out
                    rows = pl.ds(half * BLK, BLK)
                    out[rows, first] = values[:, :BLK]
                    out[rows, second] = values[:, BLK:]
                else:
                    down_out[first, half * 256 : (half + 1) * 256] = values
            return carry

        lax.fori_loop(0, HBLOCKS, step, 0)

    for pair in range(3):
        first_half(2 * pair)
        if pair < 2:
            second_half(2 * pair + 1)
        else:
            finish(2 * pair + 1)


def flush(gate_mixed, up_mixed, down_mixed, gate_out, up_out, down_out, sem):
    pairs = ((gate_mixed, gate_out), (up_mixed, up_out), (down_mixed, down_out))
    copies = [pltpu.make_async_copy(a, b, sem.at[i]) for i, (a, b) in enumerate(pairs)]
    for c in copies:
        c.start()
    for c in copies:
        c.wait()


def on_device(
    gate_weight,
    up_weight,
    down_weight,
    gate_row_bits,
    gate_col_bits,
    up_row_bits,
    up_col_bits,
    down_row_bits,
    down_col_bits,
    block_order,
):
    wide = pltpu.VMEM((LANES, HBLOCKS) + CHUNK, jnp.float32)
    square = pltpu.VMEM((256, 256), jnp.bfloat16)
    vmem = pl.BlockSpec(memory_space=pltpu.VMEM)
    hbm = pl.BlockSpec(memory_space=pl.ANY)
    weights = (gate_weight, up_weight, down_weight)
    shapes = tuple(jax.ShapeDtypeStruct(w.shape, jnp.bfloat16) for w in weights)
    mixed = pl.pallas_call(
        kernel,
        out_shape=tuple(pltpu.VMEM(w.shape, jnp.bfloat16) for w in weights),
        in_specs=[pl.BlockSpec(memory_space=pltpu.SMEM)] + [vmem] * 6 + [hbm] * 3,
        out_specs=(vmem,) * 3,
        scratch_shapes=[wide] * 9
        + [pltpu.VMEM(w.shape, jnp.bfloat16) for w in weights]
        + [square] * 3
        + [pltpu.VMEM((2, 256, 256), jnp.bfloat16)]
        + [
            pltpu.SemaphoreType.DMA((3,)),
            pltpu.SemaphoreType.DMA((SLOTS, LANES, HBLOCKS)),
            pltpu.SemaphoreType.DMA((SLOTS, LANES, HBLOCKS)),
            pltpu.SemaphoreType.DMA((LANES, HBLOCKS)),
            pltpu.SemaphoreType.DMA((LANES, HBLOCKS)),
        ],
        compiler_params=pltpu.CompilerParams(
            collective_id=0, has_side_effects=True, vmem_limit_bytes=VMEM_LIMIT
        ),
    )(
        block_order,
        gate_row_bits.reshape(1, -1),
        gate_col_bits.reshape(-1, BLK),
        up_row_bits.reshape(1, -1),
        up_col_bits.reshape(-1, BLK),
        down_row_bits.reshape(-1, BLK),
        down_col_bits.reshape(1, -1),
        *weights,
    )
    return pl.pallas_call(
        flush,
        out_shape=shapes,
        in_specs=[vmem] * 3,
        out_specs=(hbm,) * 3,
        scratch_shapes=[pltpu.SemaphoreType.DMA((3,))],
    )(*(pltpu.with_memory_space_constraint(m, pltpu.VMEM) for m in mixed))


def solution(mesh):
    return jax.shard_map(
        on_device,
        mesh=mesh,
        in_specs=(
            P("row", "col"),
            P("row", "col"),
            P("row", "col"),
            P("row"),
            P("col"),
            P("row"),
            P("col"),
            P("row"),
            P("col"),
            P(),
        ),
        out_specs=(P("row", "col"), P("row", "col"), P("row", "col")),
        check_vma=False,
    )
```

```python
import jax
import jax.numpy as jnp
from jax import lax
from jax.experimental import pallas as pl
from jax.experimental.pallas import tpu as pltpu
from jax.sharding import PartitionSpec as P

D = 4096
BLK = 128
GROUPS = 16
HBLOCKS = 7
FACTOR = (D * GROUPS * BLK) ** (-0.5)
MESH = pl.DeviceIdType.MESH
LANES = 6
SLOTS = 6
CHUNK = (128, 256)
CORE_AFTER = (1, 1, 1, 3, 3, 3)
RIGHT_AFTER = (3, 3, 3, 1, 1, 1)
VMEM_LIMIT = 55 * 1024 * 1024


def sylvester(order_size):
    rows = lax.broadcasted_iota(jnp.int32, (order_size, order_size), 0)
    both = jnp.bitwise_and(rows, lax.broadcasted_iota(jnp.int32, rows.shape, 1))
    for shift in (4, 2, 1):
        both = jnp.bitwise_xor(both, jnp.right_shift(both, shift))
    return (1 - 2 * jnp.bitwise_and(both, 1)).astype(jnp.float32)


def signs_of(bits):
    return (1 - 2 * bits).astype(jnp.float32)


def split(values):
    high = values.astype(jnp.bfloat16)
    return high, (values - high.astype(jnp.float32)).astype(jnp.bfloat16)


def dot(left, right):
    return jnp.dot(left, right, preferred_element_type=jnp.float32)


def kernel(
    gate_row_hbm,
    gate_col_hbm,
    up_row_hbm,
    up_col_hbm,
    down_row_hbm,
    down_col_hbm,
    gate_hbm,
    up_hbm,
    down_hbm,
    order_hbm,
    gate_out,
    up_out,
    down_out,
    order_out,
    own,
    got0,
    got1,
    got2,
    got3,
    got4,
    got5,
    got_core,
    sent,
    gate_in,
    up_in,
    down_in,
    gate_row,
    gate_col,
    up_row,
    up_col,
    down_row,
    down_col,
    plain,
    gate_left,
    up_left,
    in_sem,
    bits_sem,
    send_sem,
    recv_sem,
    core_send_sem,
    core_recv_sem,
):
    got = (got0, got1, got2, got3, got4, got5)
    row, col = lax.axis_index("row"), lax.axis_index("col")
    core = lax.rem(row, 2)
    x = lax.rem(lax.div(row, 2), 4)
    z_lo = lax.div(row, 8)
    y = lax.rem(col, 4)
    z_hi = lax.div(col, 4)

    def flip(bit):
        return 1 - bit

    def place(z_lo, x, core, z_hi, y):
        return (z_lo * 8 + x * 2 + core, z_hi * 4 + y)

    def one(v):
        return v + 1 - 2 * lax.rem(v, 2)

    partners = (
        (place(z_lo, one(x), core, z_hi, y), place(z_lo, 3 - x, core, z_hi, y)),
        (place(z_lo, x, core, z_hi, one(y)), place(z_lo, x, core, z_hi, 3 - y)),
        (place(flip(z_lo), x, core, z_hi, y), place(flip(z_lo), x, core, flip(z_hi), y)),
    )
    core_partner = place(z_lo, x, flip(core), z_hi, y)

    def as_sign(bit):
        return (1 - 2 * bit).astype(jnp.float32)

    low = (as_sign(lax.rem(x, 2)), as_sign(lax.rem(y, 2)), as_sign(z_lo))
    high = (as_sign(lax.div(x, 2)), as_sign(lax.div(y, 2)), as_sign(z_hi))
    core_sign = as_sign(core)

    def axis_of(group, slot):
        return (group // 2 + slot // 2) % 3

    def partner(group, slot):
        return partners[axis_of(group, slot)][(slot + group) % 2]

    def spare(slot):
        return got[slot - 2] if slot else sent

    def source(group, slot):
        if slot == 0:
            return own
        if slot % 2 == 1:
            return spare(slot - 1)
        return got_core if CORE_AFTER[group] == slot - 1 else got[slot - 1]

    def copy(group, slot, chunk):
        return pltpu.make_async_remote_copy(
            src_ref=source(group, slot).at[group, chunk],
            dst_ref=got[slot].at[group, chunk],
            send_sem=send_sem.at[slot % 2, chunk],
            recv_sem=recv_sem.at[slot, chunk],
            device_id=partner(group, slot),
            device_id_type=MESH,
        )

    def wait_all(slot, chunk):
        every = pltpu.make_async_remote_copy(
            src_ref=got[slot].at[:, chunk],
            dst_ref=got[slot].at[:, chunk],
            send_sem=send_sem.at[slot % 2, chunk],
            recv_sem=recv_sem.at[slot, chunk],
            device_id=core_partner,
            device_id_type=MESH,
        )
        every.wait_recv()
        every.wait_send()

    def core_copy(group, chunk):
        return pltpu.make_async_remote_copy(
            src_ref=got[CORE_AFTER[group]].at[group, chunk],
            dst_ref=got_core.at[group, chunk],
            send_sem=core_send_sem.at[chunk],
            recv_sem=core_recv_sem.at[group // 3, chunk],
            device_id=core_partner,
            device_id_type=MESH,
        )

    def wait_core(slot, chunk):
        half = slot // 2
        part = got_core.at[3 * half : 3 * half + 3, chunk]
        every = pltpu.make_async_remote_copy(
            src_ref=part,
            dst_ref=part,
            send_sem=core_send_sem.at[chunk],
            recv_sem=core_recv_sem.at[half, chunk],
            device_id=core_partner,
            device_id_type=MESH,
        )
        every.wait_recv()
        every.wait_send()

    barrier = pltpu.get_barrier_semaphore()
    for pair in partners:
        for device in pair:
            pl.semaphore_signal(barrier, inc=1, device_id=device, device_id_type=MESH)
    pl.semaphore_signal(barrier, inc=1, device_id=core_partner, device_id_type=MESH)

    def columns(source, target, half, first, blocks):
        lanes = pl.ds((half * HBLOCKS + first) * BLK, blocks * BLK)
        return source.at[:, lanes], target.at[:, lanes]

    def blocks(first, count):
        rows = pl.ds(first * BLK, count * BLK)
        return (
            *(columns(gate_hbm, gate_in, half, first, count) for half in range(2)),
            *(columns(up_hbm, up_in, half, first, count) for half in range(2)),
            (down_hbm.at[rows], down_in.at[rows]),
        )

    bit_loads = [
        pltpu.make_async_copy(source, target, bits_sem.at[i])
        for i, (source, target) in enumerate(
            (
                (gate_row_hbm, gate_row),
                (gate_col_hbm, gate_col),
                (up_row_hbm, up_row),
                (up_col_hbm, up_col),
                (down_row_hbm, down_row),
                (down_col_hbm, down_col),
                (order_hbm, order_out),
            )
        )
    ]
    loads = [
        [
            pltpu.make_async_copy(source, target, in_sem.at[part, i])
            for i, (source, target) in enumerate(pairs)
        ]
        for part, pairs in enumerate((blocks(0, 1), blocks(1, HBLOCKS - 1)))
    ]
    for load in bit_loads + loads[0] + loads[1]:
        load.start()

    hadamard = sylvester(2 * BLK)
    plain[...] = hadamard.astype(jnp.bfloat16)
    for load in bit_loads:
        load.wait()
    gate_left[...] = (hadamard * signs_of(gate_row[...])).astype(jnp.bfloat16)
    up_left[...] = (hadamard * signs_of(up_row[...])).astype(jnp.bfloat16)

    def block_of(chunk):
        if isinstance(chunk, int):
            return pl.ds(chunk * BLK, BLK), pl.ds((chunk + HBLOCKS) * BLK, BLK)
        return (
            pl.ds(pl.multiple_of(chunk * BLK, BLK), BLK),
            pl.ds(pl.multiple_of((chunk + HBLOCKS) * BLK, BLK), BLK),
        )

    def mix_in(weights, left, col_bits, group, chunk):
        for half, lanes in enumerate(block_of(chunk)):
            bits = col_bits[pl.ds(chunk + half * HBLOCKS, 1), :]
            mixed = dot(left[...], weights[:, lanes]) * signs_of(bits)
            out = pl.ds(half * BLK, BLK)
            own[group, chunk, :, out] = mixed[:BLK]
            own[group + 1, chunk, :, out] = mixed[BLK:]

    def mix_down(chunk):
        rows = block_of(chunk)[0]
        left = plain[:BLK, :BLK].astype(jnp.float32) * signs_of(down_row[pl.ds(chunk, 1), :])
        mixed = dot(left.astype(jnp.bfloat16), down_in[rows, :]) * signs_of(down_col[...])
        own[4, chunk] = mixed[:, :256] + mixed[:, 256:]
        own[5, chunk] = mixed[:, :256] - mixed[:, 256:]

    def mix_right(values):
        upper, lower = split(values)
        return dot(upper, plain[...]) + dot(lower, plain[...])

    def spread(chunk, carry, waits=False):
        if waits:
            loads[0][0].wait()
            loads[0][1].wait()
        mix_in(gate_in, gate_left, gate_col, 0, chunk)
        if waits:
            loads[0][2].wait()
            loads[0][3].wait()
        mix_in(up_in, up_left, up_col, 2, chunk)
        if waits:
            pl.semaphore_wait(barrier, 7)
        copy(0, 0, chunk).start()
        copy(1, 0, chunk).start()
        if waits:
            loads[0][4].wait()
        mix_down(chunk)
        copy(2, 0, chunk).start()
        copy(3, 0, chunk).start()
        if waits:
            for load in loads[1]:
                load.wait()
        copy(4, 0, chunk).start()
        copy(5, 0, chunk).start()
        return carry

    spread(0, 0, waits=True)
    lax.fori_loop(1, HBLOCKS, spread, 0)

    def first_half(slot):
        def step(chunk, carry):
            wait_all(slot, chunk)
            for group in range(LANES):
                axis = axis_of(group, slot)
                q = low[axis] if group % 2 == 0 else low[axis] * high[axis]
                mine = source(group, slot)[group, chunk]
                theirs = q * got[slot][group, chunk]
                got[slot][group, chunk] = mine + theirs
                spare(slot)[group, chunk] = mine - theirs
                if group > 0:
                    copy(group - 1, slot + 1, chunk).start()
            copy(LANES - 1, slot + 1, chunk).start()
            return carry

        lax.fori_loop(0, HBLOCKS, step, 0)

    def combined(group, slot, chunk, scale):
        axis = axis_of(group, slot)
        fk = low[axis] * high[axis] * scale
        fr = scale if group % 2 == 0 else high[axis] * scale
        return fr * got[slot][group, chunk] + fk * got[slot - 1][group, chunk]

    def second_half(slot):
        with_core = [group for group in range(LANES) if CORE_AFTER[group] == slot]
        others = [group for group in range(LANES) if CORE_AFTER[group] != slot]

        def step(chunk, carry):
            @pl.when(chunk < HBLOCKS)
            def _():
                wait_all(slot, chunk)
                ready = None
                for group in with_core + others:
                    values = combined(group, slot, chunk, 1.0)
                    if RIGHT_AFTER[group] == slot:
                        values = mix_right(values)
                    got[slot][group, chunk] = values
                    if ready is not None:
                        ready.start()
                    if group in with_core:
                        ready = core_copy(group, chunk)
                    else:
                        ready = copy(group, slot + 1, chunk)
                ready.start()

            @pl.when(chunk > 0)
            def _():
                last = chunk - 1
                wait_core(slot, last)
                ready = None
                for group in with_core:
                    got_core[group, last] = (
                        got_core[group, last] + core_sign * got[slot][group, last]
                    )
                    if ready is not None:
                        ready.start()
                    ready = copy(group, slot + 1, last)
                ready.start()

            return carry

        lax.fori_loop(0, HBLOCKS + 1, step, 0)

    def finish(slot):
        def step(chunk, carry):
            wait_all(slot, chunk)
            for group in range(LANES):
                values = combined(group, slot, chunk, FACTOR).astype(jnp.bfloat16)
                out = (gate_out, up_out, down_out)[group // 2]
                part = pl.ds((group % 2) * CHUNK[group // 4], CHUNK[group // 4])
                if group < 4:
                    out[chunk, part, :] = values
                else:
                    out[chunk, :, part] = values
            return carry

        lax.fori_loop(0, HBLOCKS, step, 0)

    for pair in range(3):
        first_half(2 * pair)
        if pair < 2:
            second_half(2 * pair + 1)
        else:
            finish(2 * pair + 1)


def flush(order_ref, gate_mixed, up_mixed, down_mixed, gate_out, up_out, down_out, sem):
    for block in range(HBLOCKS):
        chosen = order_ref[block]
        for index, mixed, out in ((0, gate_mixed, gate_out), (1, up_mixed, up_out)):
            for half in range(2):
                pltpu.make_async_copy(
                    mixed.at[chosen, :, pl.ds(half * BLK, BLK)],
                    out.at[:, pl.ds((half * HBLOCKS + block) * BLK, BLK)],
                    sem.at[index],
                ).start()
        pltpu.make_async_copy(
            down_mixed.at[chosen], down_out.at[pl.ds(block * BLK, BLK)], sem.at[2]
        ).start()
    for index, out in enumerate((gate_out, up_out, down_out)):
        pltpu.make_async_copy(out, out, sem.at[index]).wait()


def on_device(
    gate_weight,
    up_weight,
    down_weight,
    gate_row_bits,
    gate_col_bits,
    up_row_bits,
    up_col_bits,
    down_row_bits,
    down_col_bits,
    block_order,
):
    wide = pltpu.VMEM((LANES, HBLOCKS) + CHUNK, jnp.float32)
    square = pltpu.VMEM((256, 256), jnp.bfloat16)
    hbm = pl.BlockSpec(memory_space=pl.ANY)
    vmem = pl.BlockSpec(memory_space=pltpu.VMEM)
    weights = (gate_weight, up_weight, down_weight)
    bits = (
        gate_row_bits.reshape(1, -1),
        gate_col_bits.reshape(-1, BLK),
        up_row_bits.reshape(1, -1),
        up_col_bits.reshape(-1, BLK),
        down_row_bits.reshape(-1, BLK),
        down_col_bits.reshape(1, -1),
    )
    in_blocks = pltpu.VMEM((HBLOCKS, 256, 256), jnp.bfloat16)
    *mixed, order = pl.pallas_call(
        kernel,
        out_shape=(in_blocks, in_blocks, pltpu.VMEM((HBLOCKS, 128, 512), jnp.bfloat16), pltpu.SMEM((HBLOCKS,), jnp.int32)),
        in_specs=[hbm] * 10,
        out_specs=(vmem,) * 3 + (pl.BlockSpec(memory_space=pltpu.SMEM),),
        scratch_shapes=[wide] * 9
        + [pltpu.VMEM(w.shape, jnp.bfloat16) for w in weights]
        + [pltpu.VMEM(b.shape, jnp.int32) for b in bits]
        + [square] * 3
        + [
            pltpu.SemaphoreType.DMA((2, 5)),
            pltpu.SemaphoreType.DMA((7,)),
            pltpu.SemaphoreType.DMA((2, HBLOCKS)),
            pltpu.SemaphoreType.DMA((SLOTS, HBLOCKS)),
            pltpu.SemaphoreType.DMA((HBLOCKS,)),
            pltpu.SemaphoreType.DMA((2, HBLOCKS)),
        ],
        compiler_params=pltpu.CompilerParams(
            collective_id=0, has_side_effects=True, vmem_limit_bytes=VMEM_LIMIT
        ),
    )(*bits, *weights, block_order)
    return pl.pallas_call(
        flush,
        out_shape=tuple(jax.ShapeDtypeStruct(w.shape, jnp.bfloat16) for w in weights),
        in_specs=[pl.BlockSpec(memory_space=pltpu.SMEM)] + [vmem] * 3,
        out_specs=(hbm,) * 3,
        scratch_shapes=[pltpu.SemaphoreType.DMA((3,))],
    )(pltpu.with_memory_space_constraint(order, pltpu.SMEM), *(pltpu.with_memory_space_constraint(m, pltpu.VMEM) for m in mixed))


def solution(mesh):
    return jax.shard_map(
        on_device,
        mesh=mesh,
        in_specs=(
            P("row", "col"),
            P("row", "col"),
            P("row", "col"),
            P("row"),
            P("col"),
            P("row"),
            P("col"),
            P("row"),
            P("col"),
            P(),
        ),
        out_specs=(P("row", "col"), P("row", "col"), P("row", "col")),
        check_vma=False,
    )
```

```python
import jax
import jax.numpy as jnp
from jax import lax
from jax.experimental import pallas as pl
from jax.experimental.pallas import tpu as pltpu
from jax.sharding import PartitionSpec as P

D = 4096
BLK = 128
GROUPS = 16
HBLOCKS = 7
FACTOR = (D * GROUPS * BLK) ** (-0.5)
MESH = pl.DeviceIdType.MESH
LANES = 6
SLOTS = 6
CHUNK = (128, 256)
UNIT = 3
CORE_AFTER = (1, 1, 1, 3, 3, 3)
RIGHT_AFTER = (3, 3, 3, 1, 1, 1)
VMEM_LIMIT = 55 * 1024 * 1024


def sylvester(order_size):
    rows = lax.broadcasted_iota(jnp.int32, (order_size, order_size), 0)
    both = jnp.bitwise_and(rows, lax.broadcasted_iota(jnp.int32, rows.shape, 1))
    for shift in (4, 2, 1):
        both = jnp.bitwise_xor(both, jnp.right_shift(both, shift))
    return (1 - 2 * jnp.bitwise_and(both, 1)).astype(jnp.float32)


def signs_of(bits):
    return (1 - 2 * bits).astype(jnp.float32)


def split(values):
    high = values.astype(jnp.bfloat16)
    return high, (values - high.astype(jnp.float32)).astype(jnp.bfloat16)


def dot(left, right):
    return jnp.dot(left, right, preferred_element_type=jnp.float32)


def kernel(
    gate_row_hbm,
    gate_col_hbm,
    up_row_hbm,
    up_col_hbm,
    down_row_hbm,
    down_col_hbm,
    gate_hbm,
    up_hbm,
    down_hbm,
    order_hbm,
    gate_out,
    up_out,
    down_out,
    order_out,
    own,
    got0,
    got1,
    got2,
    got3,
    got4,
    got5,
    got_core,
    sent,
    in_pair,
    down_in,
    in_rows,
    in_cols,
    down_row,
    down_col,
    plain,
    gate_left,
    up_left,
    in_sem,
    bits_sem,
    send_sem,
    recv_sem,
    core_send_sem,
    core_recv_sem,
):
    got = (got0, got1, got2, got3, got4, got5)
    row, col = lax.axis_index("row"), lax.axis_index("col")
    core = lax.rem(row, 2)
    x = lax.rem(lax.div(row, 2), 4)
    z_lo = lax.div(row, 8)
    y = lax.rem(col, 4)
    z_hi = lax.div(col, 4)

    def flip(bit):
        return 1 - bit

    def place(z_lo, x, core, z_hi, y):
        return (z_lo * 8 + x * 2 + core, z_hi * 4 + y)

    def one(v):
        return v + 1 - 2 * lax.rem(v, 2)

    partners = (
        (place(z_lo, one(x), core, z_hi, y), place(z_lo, 3 - x, core, z_hi, y)),
        (place(z_lo, x, core, z_hi, one(y)), place(z_lo, x, core, z_hi, 3 - y)),
        (place(flip(z_lo), x, core, z_hi, y), place(flip(z_lo), x, core, flip(z_hi), y)),
    )
    core_partner = place(z_lo, x, flip(core), z_hi, y)

    def as_sign(bit):
        return (1 - 2 * bit).astype(jnp.float32)

    low = (as_sign(lax.rem(x, 2)), as_sign(lax.rem(y, 2)), as_sign(z_lo))
    high = (as_sign(lax.div(x, 2)), as_sign(lax.div(y, 2)), as_sign(z_hi))
    core_sign = as_sign(core)

    def axis_of(group, slot):
        return (group // 2 + slot // 2) % 3

    def partner(group, slot):
        return partners[axis_of(group, slot)][(slot + group) % 2]

    def spare(slot):
        return got[slot - 2] if slot else sent

    def source(group, slot):
        if slot == 0:
            return own
        if slot % 2 == 1:
            return spare(slot - 1)
        return got_core if CORE_AFTER[group] == slot - 1 else got[slot - 1]

    def unit_of(chunk):
        return chunk // UNIT if isinstance(chunk, int) else lax.div(chunk, UNIT)

    def copy(group, slot, chunk):
        return pltpu.make_async_remote_copy(
            src_ref=source(group, slot).at[group, chunk],
            dst_ref=got[slot].at[group, chunk],
            send_sem=send_sem.at[slot % 2],
            recv_sem=recv_sem.at[slot, unit_of(chunk)],
            device_id=partner(group, slot),
            device_id_type=MESH,
        )

    def await_chunks(slot, chunk, count):
        part = got[slot].at[:, pl.ds(chunk, count)]
        pltpu.make_async_remote_copy(
            src_ref=part,
            dst_ref=part,
            send_sem=send_sem.at[slot % 2],
            recv_sem=recv_sem.at[slot, unit_of(chunk)],
            device_id=core_partner,
            device_id_type=MESH,
        ).wait_recv()

    def await_sends(slot):
        pltpu.make_async_remote_copy(
            src_ref=got[slot],
            dst_ref=got[slot],
            send_sem=send_sem.at[slot % 2],
            recv_sem=recv_sem.at[slot, 0],
            device_id=core_partner,
            device_id_type=MESH,
        ).wait_send()

    def arrive(slot, chunk):
        @pl.when((lax.rem(chunk, UNIT) == 0) & (chunk < HBLOCKS - 1))
        def _():
            await_chunks(slot, chunk, UNIT)

        @pl.when(chunk == HBLOCKS - 1)
        def _():
            await_chunks(slot, chunk, 1)

        if slot > 0:

            @pl.when(chunk == 0)
            def _():
                await_sends(slot - 1)

    def core_copy(group, chunk):
        return pltpu.make_async_remote_copy(
            src_ref=got[CORE_AFTER[group]].at[group, chunk],
            dst_ref=got_core.at[group, chunk],
            send_sem=core_send_sem.at[0],
            recv_sem=core_recv_sem.at[group // 3, unit_of(chunk)],
            device_id=core_partner,
            device_id_type=MESH,
        )

    def await_core(slot, part, recv_unit):
        every = pltpu.make_async_remote_copy(
            src_ref=part,
            dst_ref=part,
            send_sem=core_send_sem.at[0],
            recv_sem=core_recv_sem.at[slot // 2, recv_unit],
            device_id=core_partner,
            device_id_type=MESH,
        )
        return every

    barrier = pltpu.get_barrier_semaphore()
    for pair in partners:
        for device in pair:
            pl.semaphore_signal(barrier, inc=1, device_id=device, device_id_type=MESH)
    pl.semaphore_signal(barrier, inc=1, device_id=core_partner, device_id_type=MESH)

    def columns(source, index, half, first, count):
        lanes = pl.ds((half * HBLOCKS + first) * BLK, count * BLK)
        into = pl.ds((first * 2 + half * count) * BLK, count * BLK)
        return source.at[:, lanes], in_pair.at[index, :, into]

    def load(first, count, sems):
        rows = pl.ds(first * BLK, count * BLK)
        copies = [
            pltpu.make_async_copy(*columns(source, index, half, first, count), sems[0])
            for index, source in enumerate((gate_hbm, up_hbm))
            for half in range(2)
        ]
        copies.append(pltpu.make_async_copy(down_hbm.at[rows], down_in.at[rows], sems[1]))
        for c in copies:
            c.start()
        pair = in_pair.at[:, :, pl.ds(2 * first * BLK, 2 * count * BLK)]
        return pltpu.make_async_copy(pair, pair, sems[0]), copies[-1]

    bit_loads = []
    for i, (sources, target) in enumerate(
        (
            ((gate_row_hbm, up_row_hbm), in_rows),
            ((gate_col_hbm, up_col_hbm), in_cols),
            ((down_row_hbm,), down_row),
            ((down_col_hbm,), down_col),
            ((order_hbm,), order_out),
        )
    ):
        for j, operand in enumerate(sources):
            into = target if len(sources) == 1 else target.at[j]
            pltpu.make_async_copy(operand, into, bits_sem.at[i]).start()
        bit_loads.append(pltpu.make_async_copy(target, target, bits_sem.at[i]))
    loads = [load(0, 1, (in_sem.at[0], in_sem.at[1]))]
    loads.append(load(1, HBLOCKS - 1, (in_sem.at[2], in_sem.at[3])))

    hadamard = sylvester(2 * BLK)
    plain[...] = hadamard.astype(jnp.bfloat16)
    for pending in bit_loads:
        pending.wait()
    gate_left[...] = (hadamard * signs_of(in_rows[0])).astype(jnp.bfloat16)
    up_left[...] = (hadamard * signs_of(in_rows[1])).astype(jnp.bfloat16)

    def mix_in(index, left, chunk):
        for half in range(2):
            if isinstance(chunk, int):
                lanes = pl.ds(half * BLK, BLK)
            else:
                lanes = pl.ds(
                    pl.multiple_of((chunk + 1 + half * (HBLOCKS - 1)) * BLK, BLK), BLK
                )
            bits = in_cols[index, pl.ds(chunk + half * HBLOCKS, 1), :]
            mixed = dot(left[...], in_pair[index, :, lanes]) * signs_of(bits)
            out = pl.ds(half * BLK, BLK)
            own[2 * index, chunk, :, out] = mixed[:BLK]
            own[2 * index + 1, chunk, :, out] = mixed[BLK:]

    def mix_down(chunk):
        first = chunk * BLK
        rows = pl.ds(first if isinstance(chunk, int) else pl.multiple_of(first, BLK), BLK)
        left = plain[:BLK, :BLK].astype(jnp.float32) * signs_of(down_row[pl.ds(chunk, 1), :])
        mixed = dot(left.astype(jnp.bfloat16), down_in[rows, :]) * signs_of(down_col[...])
        own[4, chunk] = mixed[:, :256] + mixed[:, 256:]
        own[5, chunk] = mixed[:, :256] - mixed[:, 256:]

    def mix_right(values):
        upper, lower = split(values)
        return dot(upper, plain[...]) + dot(lower, plain[...])

    def spread(chunk, carry, waits=False):
        if waits:
            loads[0][0].wait()
        mix_in(0, gate_left, chunk)
        mix_in(1, up_left, chunk)
        if waits:
            pl.semaphore_wait(barrier, 7)
        copy(0, 0, chunk).start()
        copy(1, 0, chunk).start()
        if waits:
            loads[0][1].wait()
        mix_down(chunk)
        copy(2, 0, chunk).start()
        copy(3, 0, chunk).start()
        if waits:
            loads[1][0].wait()
            loads[1][1].wait()
        copy(4, 0, chunk).start()
        copy(5, 0, chunk).start()
        return carry

    spread(0, 0, waits=True)
    lax.fori_loop(1, HBLOCKS, spread, 0)

    def first_half(slot):
        def step(chunk, carry):
            arrive(slot, chunk)
            for group in range(LANES):
                axis = axis_of(group, slot)
                q = low[axis] if group % 2 == 0 else low[axis] * high[axis]
                mine = source(group, slot)[group, chunk]
                theirs = q * got[slot][group, chunk]
                got[slot][group, chunk] = mine + theirs
                spare(slot)[group, chunk] = mine - theirs
                if group > 0:
                    copy(group - 1, slot + 1, chunk).start()
            copy(LANES - 1, slot + 1, chunk).start()
            return carry

        lax.fori_loop(0, HBLOCKS, step, 0)

    def combined(group, slot, chunk, scale):
        axis = axis_of(group, slot)
        fk = low[axis] * high[axis] * scale
        fr = scale if group % 2 == 0 else high[axis] * scale
        return fr * got[slot][group, chunk] + fk * got[slot - 1][group, chunk]

    def second_half(slot):
        with_core = [group for group in range(LANES) if CORE_AFTER[group] == slot]
        others = [group for group in range(LANES) if CORE_AFTER[group] != slot]

        def settle(first, count):
            part = got_core.at[pl.ds(with_core[0], 3), pl.ds(first, count)]
            await_core(slot, part, unit_of(first)).wait_recv()

            def one_chunk(index, carry):
                last = first + index
                ready = None
                for group in with_core:
                    got_core[group, last] = (
                        got_core[group, last] + core_sign * got[slot][group, last]
                    )
                    if ready is not None:
                        ready.start()
                    ready = copy(group, slot + 1, last)
                ready.start()
                return carry

            lax.fori_loop(0, count, one_chunk, 0)

        def step(chunk, carry):
            arrive(slot, chunk)
            ready = None
            for group in with_core + others:
                values = combined(group, slot, chunk, 1.0)
                if RIGHT_AFTER[group] == slot:
                    values = mix_right(values)
                got[slot][group, chunk] = values
                if ready is not None:
                    ready.start()
                if group in with_core:
                    ready = core_copy(group, chunk)
                else:
                    ready = copy(group, slot + 1, chunk)
            ready.start()

            @pl.when(lax.rem(chunk, UNIT) == UNIT - 1)
            def _():
                settle(chunk - (UNIT - 1), UNIT)

            @pl.when(chunk == HBLOCKS - 1)
            def _():
                settle(chunk, 1)

            return carry

        lax.fori_loop(0, HBLOCKS, step, 0)
        await_core(slot, got_core.at[pl.ds(with_core[0], 3)], 0).wait_send()

    def finish(slot):
        def step(chunk, carry):
            arrive(slot, chunk)
            for group in range(LANES):
                values = combined(group, slot, chunk, FACTOR).astype(jnp.bfloat16)
                out = (gate_out, up_out, down_out)[group // 2]
                part = pl.ds((group % 2) * CHUNK[group // 4], CHUNK[group // 4])
                if group < 4:
                    out[chunk, part, :] = values
                else:
                    out[chunk, :, part] = values
            return carry

        lax.fori_loop(0, HBLOCKS, step, 0)
        await_sends(slot)

    for pair in range(3):
        first_half(2 * pair)
        if pair < 2:
            second_half(2 * pair + 1)
        else:
            finish(2 * pair + 1)


def flush(order_ref, gate_mixed, up_mixed, down_mixed, gate_out, up_out, down_out, sem):
    for block in range(HBLOCKS):
        chosen = order_ref[block]
        for index, mixed, out in ((0, gate_mixed, gate_out), (1, up_mixed, up_out)):
            for half in range(2):
                pltpu.make_async_copy(
                    mixed.at[chosen, :, pl.ds(half * BLK, BLK)],
                    out.at[:, pl.ds((half * HBLOCKS + block) * BLK, BLK)],
                    sem.at[index],
                ).start()
        pltpu.make_async_copy(
            down_mixed.at[chosen], down_out.at[pl.ds(block * BLK, BLK)], sem.at[2]
        ).start()
    for index, out in enumerate((gate_out, up_out, down_out)):
        pltpu.make_async_copy(out, out, sem.at[index]).wait()


def on_device(
    gate_weight,
    up_weight,
    down_weight,
    gate_row_bits,
    gate_col_bits,
    up_row_bits,
    up_col_bits,
    down_row_bits,
    down_col_bits,
    block_order,
):
    wide = pltpu.VMEM((LANES, HBLOCKS) + CHUNK, jnp.float32)
    square = pltpu.VMEM((256, 256), jnp.bfloat16)
    hbm = pl.BlockSpec(memory_space=pl.ANY)
    vmem = pl.BlockSpec(memory_space=pltpu.VMEM)
    weights = (gate_weight, up_weight, down_weight)
    bits = (
        gate_row_bits.reshape(1, -1),
        gate_col_bits.reshape(-1, BLK),
        up_row_bits.reshape(1, -1),
        up_col_bits.reshape(-1, BLK),
        down_row_bits.reshape(-1, BLK),
        down_col_bits.reshape(1, -1),
    )
    in_blocks = pltpu.VMEM((HBLOCKS, 256, 256), jnp.bfloat16)
    *mixed, order = pl.pallas_call(
        kernel,
        out_shape=(in_blocks, in_blocks, pltpu.VMEM((HBLOCKS, 128, 512), jnp.bfloat16), pltpu.SMEM((HBLOCKS,), jnp.int32)),
        in_specs=[hbm] * 10,
        out_specs=(vmem,) * 3 + (pl.BlockSpec(memory_space=pltpu.SMEM),),
        scratch_shapes=[wide] * 9
        + [
            pltpu.VMEM((2,) + gate_weight.shape, jnp.bfloat16),
            pltpu.VMEM(down_weight.shape, jnp.bfloat16),
            pltpu.VMEM((2,) + bits[0].shape, jnp.int32),
            pltpu.VMEM((2,) + bits[1].shape, jnp.int32),
            pltpu.VMEM(bits[4].shape, jnp.int32),
            pltpu.VMEM(bits[5].shape, jnp.int32),
        ]
        + [square] * 3
        + [
            pltpu.SemaphoreType.DMA((4,)),
            pltpu.SemaphoreType.DMA((5,)),
            pltpu.SemaphoreType.DMA((2,)),
            pltpu.SemaphoreType.DMA((SLOTS, -(-HBLOCKS // UNIT))),
            pltpu.SemaphoreType.DMA((1,)),
            pltpu.SemaphoreType.DMA((2, -(-HBLOCKS // UNIT))),
        ],
        compiler_params=pltpu.CompilerParams(
            collective_id=0, has_side_effects=True, vmem_limit_bytes=VMEM_LIMIT
        ),
    )(*bits, *weights, block_order)
    return pl.pallas_call(
        flush,
        out_shape=tuple(jax.ShapeDtypeStruct(w.shape, jnp.bfloat16) for w in weights),
        in_specs=[pl.BlockSpec(memory_space=pltpu.SMEM)] + [vmem] * 3,
        out_specs=(hbm,) * 3,
        scratch_shapes=[pltpu.SemaphoreType.DMA((3,))],
    )(pltpu.with_memory_space_constraint(order, pltpu.SMEM), *(pltpu.with_memory_space_constraint(m, pltpu.VMEM) for m in mixed))


def solution(mesh):
    return jax.shard_map(
        on_device,
        mesh=mesh,
        in_specs=(
            P("row", "col"),
            P("row", "col"),
            P("row", "col"),
            P("row"),
            P("col"),
            P("row"),
            P("col"),
            P("row"),
            P("col"),
            P(),
        ),
        out_specs=(P("row", "col"), P("row", "col"), P("row", "col")),
        check_vma=False,
    )
```

```python
import jax
import jax.numpy as jnp
from jax import lax
from jax.experimental import pallas as pl
from jax.experimental.pallas import tpu as pltpu
from jax.sharding import PartitionSpec as P

D = 4096
BLK = 128
GROUPS = 16
HBLOCKS = 7
FACTOR = (D * GROUPS * BLK) ** (-0.5)
MESH = pl.DeviceIdType.MESH
LANES = 6
SLOTS = 6
CHUNK = (128, 256)
UNIT = 3
CORE_AFTER = (1, 1, 1, 3, 3, 3)
RIGHT_AFTER = (3, 3, 3, 1, 1, 1)
VMEM_LIMIT = 55 * 1024 * 1024


def sylvester(order_size):
    rows = lax.broadcasted_iota(jnp.int32, (order_size, order_size), 0)
    both = jnp.bitwise_and(rows, lax.broadcasted_iota(jnp.int32, rows.shape, 1))
    for shift in (4, 2, 1):
        both = jnp.bitwise_xor(both, jnp.right_shift(both, shift))
    return (1 - 2 * jnp.bitwise_and(both, 1)).astype(jnp.float32)


def signs_of(bits):
    return (1 - 2 * bits).astype(jnp.float32)


def split(values):
    high = values.astype(jnp.bfloat16)
    return high, (values - high.astype(jnp.float32)).astype(jnp.bfloat16)


def dot(left, right):
    return jnp.dot(left, right, preferred_element_type=jnp.float32)


def kernel(
    gate_row_hbm,
    gate_col_hbm,
    up_row_hbm,
    up_col_hbm,
    down_row_hbm,
    down_col_hbm,
    gate_hbm,
    up_hbm,
    down_hbm,
    order_hbm,
    gate_out,
    up_out,
    down_out,
    order_out,
    own,
    got0,
    got1,
    got2,
    got3,
    got4,
    got5,
    got_core,
    sent,
    in_pair,
    down_in,
    in_rows,
    in_cols,
    down_row,
    down_col,
    plain,
    gate_left,
    up_left,
    in_sem,
    bits_sem,
    send_sem,
    recv_sem,
    core_send_sem,
    core_recv_sem,
    ready,
):
    got = (got0, got1, got2, got3, got4, got5)
    row, col = lax.axis_index("row"), lax.axis_index("col")
    core = lax.rem(row, 2)
    x = lax.rem(lax.div(row, 2), 4)
    z_lo = lax.div(row, 8)
    y = lax.rem(col, 4)
    z_hi = lax.div(col, 4)

    def flip(bit):
        return 1 - bit

    def place(z_lo, x, core, z_hi, y):
        return (z_lo * 8 + x * 2 + core, z_hi * 4 + y)

    def one(v):
        return v + 1 - 2 * lax.rem(v, 2)

    partners = (
        (place(z_lo, one(x), core, z_hi, y), place(z_lo, 3 - x, core, z_hi, y)),
        (place(z_lo, x, core, z_hi, one(y)), place(z_lo, x, core, z_hi, 3 - y)),
        (place(flip(z_lo), x, core, z_hi, y), place(flip(z_lo), x, core, flip(z_hi), y)),
    )
    core_partner = place(z_lo, x, flip(core), z_hi, y)

    def as_sign(bit):
        return (1 - 2 * bit).astype(jnp.float32)

    low = (as_sign(lax.rem(x, 2)), as_sign(lax.rem(y, 2)), as_sign(z_lo))
    high = (as_sign(lax.div(x, 2)), as_sign(lax.div(y, 2)), as_sign(z_hi))
    core_sign = as_sign(core)

    def axis_of(group, slot):
        return (group // 2 + slot // 2) % 3

    def partner(group, slot):
        return partners[axis_of(group, slot)][(slot + group) % 2]

    def spare(slot):
        return got[slot - 2] if slot else sent

    def source(group, slot):
        if slot == 0:
            return own
        if slot % 2 == 1:
            return spare(slot - 1)
        return got_core if CORE_AFTER[group] == slot - 1 else got[slot - 1]

    def unit_of(chunk):
        return chunk // UNIT if isinstance(chunk, int) else lax.div(chunk, UNIT)

    def copy(group, slot, chunk):
        return pltpu.make_async_remote_copy(
            src_ref=source(group, slot).at[group, chunk],
            dst_ref=got[slot].at[group, chunk],
            send_sem=send_sem.at[slot % 2],
            recv_sem=recv_sem.at[slot, unit_of(chunk)],
            device_id=partner(group, slot),
            device_id_type=MESH,
        )

    def await_chunks(slot, chunk, count):
        part = got[slot].at[:, pl.ds(chunk, count)]
        pltpu.make_async_remote_copy(
            src_ref=part,
            dst_ref=part,
            send_sem=send_sem.at[slot % 2],
            recv_sem=recv_sem.at[slot, unit_of(chunk)],
            device_id=core_partner,
            device_id_type=MESH,
        ).wait_recv()

    def await_sends(slot):
        pltpu.make_async_remote_copy(
            src_ref=got[slot],
            dst_ref=got[slot],
            send_sem=send_sem.at[slot % 2],
            recv_sem=recv_sem.at[slot, 0],
            device_id=core_partner,
            device_id_type=MESH,
        ).wait_send()

    def arrive(slot, chunk):
        @pl.when((lax.rem(chunk, UNIT) == 0) & (chunk < HBLOCKS - 1))
        def _():
            await_chunks(slot, chunk, UNIT)

        @pl.when(chunk == HBLOCKS - 1)
        def _():
            await_chunks(slot, chunk, 1)

        if slot > 0:

            @pl.when(chunk == 0)
            def _():
                await_sends(slot - 1)

    def core_copy(group, chunk):
        return pltpu.make_async_remote_copy(
            src_ref=got[CORE_AFTER[group]].at[group, chunk],
            dst_ref=got_core.at[group, chunk],
            send_sem=core_send_sem.at[0],
            recv_sem=core_recv_sem.at[group // 3, unit_of(chunk)],
            device_id=core_partner,
            device_id_type=MESH,
        )

    def await_core(slot, part, recv_unit):
        every = pltpu.make_async_remote_copy(
            src_ref=part,
            dst_ref=part,
            send_sem=core_send_sem.at[0],
            recv_sem=core_recv_sem.at[slot // 2, recv_unit],
            device_id=core_partner,
            device_id_type=MESH,
        )
        return every

    barrier = pltpu.get_barrier_semaphore()
    links = [(bits[axis], partners[axis][kind]) for axis in range(3) for kind, bits in enumerate(
        ((lax.rem(x, 2), lax.rem(y, 2), z_lo), (lax.div(x, 2), lax.div(y, 2), z_hi))
    )]
    links.append((flip(core), core_partner))
    for is_higher, device in links:

        @pl.when(is_higher == 0)
        def _(device=device):
            pl.semaphore_signal(barrier, inc=1, device_id=device, device_id_type=MESH)

    def columns(source, index, half, first, count):
        lanes = pl.ds((half * HBLOCKS + first) * BLK, count * BLK)
        into = pl.ds((first * 2 + half * count) * BLK, count * BLK)
        return source.at[:, lanes], in_pair.at[index, :, into]

    def load(first, count, sems):
        rows = pl.ds(first * BLK, count * BLK)
        copies = [
            pltpu.make_async_copy(*columns(source, index, half, first, count), sems[0])
            for index, source in enumerate((gate_hbm, up_hbm))
            for half in range(2)
        ]
        copies.append(pltpu.make_async_copy(down_hbm.at[rows], down_in.at[rows], sems[1]))
        for c in copies:
            c.start()
        pair = in_pair.at[:, :, pl.ds(2 * first * BLK, 2 * count * BLK)]
        return pltpu.make_async_copy(pair, pair, sems[0]), copies[-1]

    bit_loads = []
    for i, (sources, target) in enumerate(
        (
            ((gate_row_hbm, up_row_hbm), in_rows),
            ((gate_col_hbm, up_col_hbm), in_cols),
            ((down_row_hbm,), down_row),
            ((down_col_hbm,), down_col),
            ((order_hbm,), order_out),
        )
    ):
        for j, operand in enumerate(sources):
            into = target if len(sources) == 1 else target.at[j]
            pltpu.make_async_copy(operand, into, bits_sem.at[i]).start()
        bit_loads.append(pltpu.make_async_copy(target, target, bits_sem.at[i]))
    loads = [load(0, 1, (in_sem.at[0], in_sem.at[1]))]
    loads.append(load(1, HBLOCKS - 1, (in_sem.at[2], in_sem.at[3])))

    hadamard = sylvester(2 * BLK)
    plain[...] = hadamard.astype(jnp.bfloat16)
    lower_ends = sum(is_higher for is_higher, _ in links)

    @pl.when(lower_ends > 0)
    def _():
        pl.semaphore_wait(barrier, lower_ends)

    for index, (is_higher, device) in enumerate(links):

        @pl.when(is_higher == 1)
        def _(index=index, device=device):
            pl.semaphore_signal(ready.at[index], inc=1, device_id=device, device_id_type=MESH)

    for pending in bit_loads:
        pending.wait()
    gate_left[...] = (hadamard * signs_of(in_rows[0])).astype(jnp.bfloat16)
    up_left[...] = (hadamard * signs_of(in_rows[1])).astype(jnp.bfloat16)

    def mix_in(index, left, chunk):
        for half in range(2):
            if isinstance(chunk, int):
                lanes = pl.ds(half * BLK, BLK)
            else:
                lanes = pl.ds(
                    pl.multiple_of((chunk + 1 + half * (HBLOCKS - 1)) * BLK, BLK), BLK
                )
            bits = in_cols[index, pl.ds(chunk + half * HBLOCKS, 1), :]
            mixed = dot(left[...], in_pair[index, :, lanes]) * signs_of(bits)
            out = pl.ds(half * BLK, BLK)
            own[2 * index, chunk, :, out] = mixed[:BLK]
            own[2 * index + 1, chunk, :, out] = mixed[BLK:]

    def mix_down(chunk):
        first = chunk * BLK
        rows = pl.ds(first if isinstance(chunk, int) else pl.multiple_of(first, BLK), BLK)
        left = plain[:BLK, :BLK].astype(jnp.float32) * signs_of(down_row[pl.ds(chunk, 1), :])
        mixed = dot(left.astype(jnp.bfloat16), down_in[rows, :]) * signs_of(down_col[...])
        own[4, chunk] = mixed[:, :256] + mixed[:, 256:]
        own[5, chunk] = mixed[:, :256] - mixed[:, 256:]

    def mix_right(values):
        upper, lower = split(values)
        return dot(upper, plain[...]) + dot(lower, plain[...])

    def send_first(chunk, groups=range(LANES)):
        for group in groups:
            copy(group, 0, chunk).start()

    def send_when_ready(groups):
        for group in groups:

            @pl.when(links[group][0] == 0)
            def _(group=group):
                pl.semaphore_wait(ready.at[group], 1)
                copy(group, 0, 0).start()

    def mix(chunk):
        mix_in(0, gate_left, chunk)
        mix_in(1, up_left, chunk)
        mix_down(chunk)

    loads[0][0].wait()
    loads[0][1].wait()
    mix(0)
    for group in range(LANES):

        @pl.when(links[group][0] == 1)
        def _(group=group):
            copy(group, 0, 0).start()

    send_when_ready(range(4))
    loads[1][0].wait()
    loads[1][1].wait()

    def spread(chunk, carry):
        mix(chunk)
        send_first(chunk)
        return carry

    def second(chunk, carry):
        mix(chunk)
        send_first(chunk, range(4))
        return carry

    lax.fori_loop(1, 2, second, 0)
    send_when_ready(range(4, LANES))
    send_first(1, range(4, LANES))

    @pl.when(core == 1)
    def _():
        pl.semaphore_wait(ready.at[LANES], 1)

    lax.fori_loop(2, HBLOCKS, spread, 0)

    def first_half(slot):
        def step(chunk, carry):
            arrive(slot, chunk)
            for group in range(LANES):
                axis = axis_of(group, slot)
                q = low[axis] if group % 2 == 0 else low[axis] * high[axis]
                mine = source(group, slot)[group, chunk]
                theirs = q * got[slot][group, chunk]
                got[slot][group, chunk] = mine + theirs
                spare(slot)[group, chunk] = mine - theirs
                if group > 0:
                    copy(group - 1, slot + 1, chunk).start()
            copy(LANES - 1, slot + 1, chunk).start()
            return carry

        lax.fori_loop(0, HBLOCKS, step, 0)

    def combined(group, slot, chunk, scale):
        axis = axis_of(group, slot)
        fk = low[axis] * high[axis] * scale
        fr = scale if group % 2 == 0 else high[axis] * scale
        return fr * got[slot][group, chunk] + fk * got[slot - 1][group, chunk]

    def second_half(slot):
        with_core = [group for group in range(LANES) if CORE_AFTER[group] == slot]
        others = [group for group in range(LANES) if CORE_AFTER[group] != slot]

        def settle(first, count):
            part = got_core.at[pl.ds(with_core[0], 3), pl.ds(first, count)]
            await_core(slot, part, unit_of(first)).wait_recv()

            def one_chunk(index, carry):
                last = first + index
                ready = None
                for group in with_core:
                    got_core[group, last] = (
                        got_core[group, last] + core_sign * got[slot][group, last]
                    )
                    if ready is not None:
                        ready.start()
                    ready = copy(group, slot + 1, last)
                ready.start()
                return carry

            lax.fori_loop(0, count, one_chunk, 0)

        def step(chunk, carry):
            arrive(slot, chunk)
            ready = None
            for group in with_core + others:
                values = combined(group, slot, chunk, 1.0)
                if RIGHT_AFTER[group] == slot:
                    values = mix_right(values)
                got[slot][group, chunk] = values
                if ready is not None:
                    ready.start()
                if group in with_core:
                    ready = core_copy(group, chunk)
                else:
                    ready = copy(group, slot + 1, chunk)
            ready.start()

            @pl.when(lax.rem(chunk, UNIT) == UNIT - 1)
            def _():
                settle(chunk - (UNIT - 1), UNIT)

            @pl.when(chunk == HBLOCKS - 1)
            def _():
                settle(chunk, 1)

            return carry

        lax.fori_loop(0, HBLOCKS, step, 0)
        await_core(slot, got_core.at[pl.ds(with_core[0], 3)], 0).wait_send()

    def finish(slot):
        def step(chunk, carry):
            arrive(slot, chunk)
            for group in range(LANES):
                values = combined(group, slot, chunk, FACTOR).astype(jnp.bfloat16)
                out = (gate_out, up_out, down_out)[group // 2]
                part = pl.ds((group % 2) * CHUNK[group // 4], CHUNK[group // 4])
                if group < 4:
                    out[chunk, part, :] = values
                else:
                    out[chunk, :, part] = values
            return carry

        lax.fori_loop(0, HBLOCKS, step, 0)
        await_sends(slot)

    for pair in range(3):
        first_half(2 * pair)
        if pair < 2:
            second_half(2 * pair + 1)
        else:
            finish(2 * pair + 1)


def flush(order_ref, gate_mixed, up_mixed, down_mixed, gate_out, up_out, down_out, sem):
    for block in range(HBLOCKS):
        chosen = order_ref[block]
        for index, mixed, out in ((0, gate_mixed, gate_out), (1, up_mixed, up_out)):
            for half in range(2):
                pltpu.make_async_copy(
                    mixed.at[chosen, :, pl.ds(half * BLK, BLK)],
                    out.at[:, pl.ds((half * HBLOCKS + block) * BLK, BLK)],
                    sem.at[index],
                ).start()
        pltpu.make_async_copy(
            down_mixed.at[chosen], down_out.at[pl.ds(block * BLK, BLK)], sem.at[2]
        ).start()
    for index, out in enumerate((gate_out, up_out, down_out)):
        pltpu.make_async_copy(out, out, sem.at[index]).wait()


def on_device(
    gate_weight,
    up_weight,
    down_weight,
    gate_row_bits,
    gate_col_bits,
    up_row_bits,
    up_col_bits,
    down_row_bits,
    down_col_bits,
    block_order,
):
    wide = pltpu.VMEM((LANES, HBLOCKS) + CHUNK, jnp.float32)
    square = pltpu.VMEM((256, 256), jnp.bfloat16)
    hbm = pl.BlockSpec(memory_space=pl.ANY)
    vmem = pl.BlockSpec(memory_space=pltpu.VMEM)
    weights = (gate_weight, up_weight, down_weight)
    bits = (
        gate_row_bits.reshape(1, -1),
        gate_col_bits.reshape(-1, BLK),
        up_row_bits.reshape(1, -1),
        up_col_bits.reshape(-1, BLK),
        down_row_bits.reshape(-1, BLK),
        down_col_bits.reshape(1, -1),
    )
    in_blocks = pltpu.VMEM((HBLOCKS, 256, 256), jnp.bfloat16)
    *mixed, order = pl.pallas_call(
        kernel,
        out_shape=(in_blocks, in_blocks, pltpu.VMEM((HBLOCKS, 128, 512), jnp.bfloat16), pltpu.SMEM((HBLOCKS,), jnp.int32)),
        in_specs=[hbm] * 10,
        out_specs=(vmem,) * 3 + (pl.BlockSpec(memory_space=pltpu.SMEM),),
        scratch_shapes=[wide] * 9
        + [
            pltpu.VMEM((2,) + gate_weight.shape, jnp.bfloat16),
            pltpu.VMEM(down_weight.shape, jnp.bfloat16),
            pltpu.VMEM((2,) + bits[0].shape, jnp.int32),
            pltpu.VMEM((2,) + bits[1].shape, jnp.int32),
            pltpu.VMEM(bits[4].shape, jnp.int32),
            pltpu.VMEM(bits[5].shape, jnp.int32),
        ]
        + [square] * 3
        + [
            pltpu.SemaphoreType.DMA((4,)),
            pltpu.SemaphoreType.DMA((5,)),
            pltpu.SemaphoreType.DMA((2,)),
            pltpu.SemaphoreType.DMA((SLOTS, -(-HBLOCKS // UNIT))),
            pltpu.SemaphoreType.DMA((1,)),
            pltpu.SemaphoreType.DMA((2, -(-HBLOCKS // UNIT))),
            pltpu.SemaphoreType.REGULAR((LANES + 1,)),
        ],
        compiler_params=pltpu.CompilerParams(
            collective_id=0, has_side_effects=True, vmem_limit_bytes=VMEM_LIMIT
        ),
    )(*bits, *weights, block_order)
    return pl.pallas_call(
        flush,
        out_shape=tuple(jax.ShapeDtypeStruct(w.shape, jnp.bfloat16) for w in weights),
        in_specs=[pl.BlockSpec(memory_space=pltpu.SMEM)] + [vmem] * 3,
        out_specs=(hbm,) * 3,
        scratch_shapes=[pltpu.SemaphoreType.DMA((3,))],
    )(pltpu.with_memory_space_constraint(order, pltpu.SMEM), *(pltpu.with_memory_space_constraint(m, pltpu.VMEM) for m in mixed))


def solution(mesh):
    return jax.shard_map(
        on_device,
        mesh=mesh,
        in_specs=(
            P("row", "col"),
            P("row", "col"),
            P("row", "col"),
            P("row"),
            P("col"),
            P("row"),
            P("col"),
            P("row"),
            P("col"),
            P(),
        ),
        out_specs=(P("row", "col"), P("row", "col"), P("row", "col")),
        check_vma=False,
    )
```

```python
import jax
import jax.numpy as jnp
from jax import lax
from jax.experimental import pallas as pl
from jax.experimental.pallas import tpu as pltpu
from jax.sharding import PartitionSpec as P

D = 4096
BLK = 128
GROUPS = 16
HBLOCKS = 7
FACTOR = (D * GROUPS * BLK) ** (-0.5)
MESH = pl.DeviceIdType.MESH
LANES = 6
SLOTS = 6
CHUNK = (128, 256)
UNIT = 3
CORE_AFTER = (1, 1, 1, 3, 3, 3)
RIGHT_AFTER = (3, 3, 3, 1, 1, 1)
VMEM_LIMIT = 55 * 1024 * 1024


def sylvester(order_size):
    rows = lax.broadcasted_iota(jnp.int32, (order_size, order_size), 0)
    both = jnp.bitwise_and(rows, lax.broadcasted_iota(jnp.int32, rows.shape, 1))
    for shift in (4, 2, 1):
        both = jnp.bitwise_xor(both, jnp.right_shift(both, shift))
    return (1 - 2 * jnp.bitwise_and(both, 1)).astype(jnp.float32)


def signs_of(bits):
    return (1 - 2 * bits).astype(jnp.float32)


def split(values):
    high = values.astype(jnp.bfloat16)
    return high, (values - high.astype(jnp.float32)).astype(jnp.bfloat16)


def dot(left, right):
    return jnp.dot(left, right, preferred_element_type=jnp.float32)


def kernel(
    gate_row_hbm,
    gate_col_hbm,
    up_row_hbm,
    up_col_hbm,
    down_row_hbm,
    down_col_hbm,
    gate_hbm,
    up_hbm,
    down_hbm,
    order_hbm,
    gate_out,
    up_out,
    down_out,
    order_out,
    own,
    got0,
    got1,
    got2,
    got3,
    got4,
    got5,
    got_core,
    sent,
    in_pair,
    down_in,
    in_rows,
    in_cols,
    down_row,
    down_col,
    plain,
    gate_left,
    up_left,
    in_sem,
    bits_sem,
    send_sem,
    recv_sem,
    core_send_sem,
    core_recv_sem,
    ready,
):
    got = (got0, got1, got2, got3, got4, got5)
    row, col = lax.axis_index("row"), lax.axis_index("col")
    core = lax.rem(row, 2)
    x = lax.rem(lax.div(row, 2), 4)
    z_lo = lax.div(row, 8)
    y = lax.rem(col, 4)
    z_hi = lax.div(col, 4)

    def flip(bit):
        return 1 - bit

    def place(z_lo, x, core, z_hi, y):
        return (z_lo * 8 + x * 2 + core, z_hi * 4 + y)

    def one(v):
        return v + 1 - 2 * lax.rem(v, 2)

    partners = (
        (place(z_lo, one(x), core, z_hi, y), place(z_lo, 3 - x, core, z_hi, y)),
        (place(z_lo, x, core, z_hi, one(y)), place(z_lo, x, core, z_hi, 3 - y)),
        (place(flip(z_lo), x, core, z_hi, y), place(flip(z_lo), x, core, flip(z_hi), y)),
    )
    core_partner = place(z_lo, x, flip(core), z_hi, y)

    def as_sign(bit):
        return (1 - 2 * bit).astype(jnp.float32)

    low = (as_sign(lax.rem(x, 2)), as_sign(lax.rem(y, 2)), as_sign(z_lo))
    high = (as_sign(lax.div(x, 2)), as_sign(lax.div(y, 2)), as_sign(z_hi))
    core_sign = as_sign(core)

    def axis_of(group, slot):
        return (group // 2 + slot // 2) % 3

    def partner(group, slot):
        return partners[axis_of(group, slot)][(slot + group) % 2]

    def spare(slot):
        return got[slot - 2] if slot else sent

    def source(group, slot):
        if slot == 0:
            return own
        if slot % 2 == 1:
            return spare(slot - 1)
        return got_core if CORE_AFTER[group] == slot - 1 else got[slot - 1]

    def unit_of(chunk):
        return chunk // UNIT if isinstance(chunk, int) else lax.div(chunk, UNIT)

    def copy(group, slot, chunk):
        return pltpu.make_async_remote_copy(
            src_ref=source(group, slot).at[group, chunk],
            dst_ref=got[slot].at[group, chunk],
            send_sem=send_sem.at[slot % 2],
            recv_sem=recv_sem.at[slot, unit_of(chunk)],
            device_id=partner(group, slot),
            device_id_type=MESH,
        )

    def await_chunks(slot, chunk, count):
        part = got[slot].at[:, pl.ds(chunk, count)]
        pltpu.make_async_remote_copy(
            src_ref=part,
            dst_ref=part,
            send_sem=send_sem.at[slot % 2],
            recv_sem=recv_sem.at[slot, unit_of(chunk)],
            device_id=core_partner,
            device_id_type=MESH,
        ).wait_recv()

    def await_sends(slot):
        pltpu.make_async_remote_copy(
            src_ref=got[slot],
            dst_ref=got[slot],
            send_sem=send_sem.at[slot % 2],
            recv_sem=recv_sem.at[slot, 0],
            device_id=core_partner,
            device_id_type=MESH,
        ).wait_send()

    def arrive(slot, chunk):
        @pl.when((lax.rem(chunk, UNIT) == 0) & (chunk < HBLOCKS - 1))
        def _():
            await_chunks(slot, chunk, UNIT)

        @pl.when(chunk == HBLOCKS - 1)
        def _():
            await_chunks(slot, chunk, 1)

        if slot > 0:

            @pl.when(chunk == 0)
            def _():
                await_sends(slot - 1)

    def core_copy(group, chunk):
        return pltpu.make_async_remote_copy(
            src_ref=got[CORE_AFTER[group]].at[group, chunk],
            dst_ref=got_core.at[group, chunk],
            send_sem=core_send_sem.at[0],
            recv_sem=core_recv_sem.at[group // 3, unit_of(chunk)],
            device_id=core_partner,
            device_id_type=MESH,
        )

    def await_core(slot, part, recv_unit):
        every = pltpu.make_async_remote_copy(
            src_ref=part,
            dst_ref=part,
            send_sem=core_send_sem.at[0],
            recv_sem=core_recv_sem.at[slot // 2, recv_unit],
            device_id=core_partner,
            device_id_type=MESH,
        )
        return every

    def columns(source, index, half, first, count):
        lanes = pl.ds((half * HBLOCKS + first) * BLK, count * BLK)
        into = pl.ds((first * 2 + half * count) * BLK, count * BLK)
        return source.at[:, lanes], in_pair.at[index, :, into]

    def load(first, count, sems):
        rows = pl.ds(first * BLK, count * BLK)
        copies = [pltpu.make_async_copy(down_hbm.at[rows], down_in.at[rows], sems[1])]
        copies += [
            pltpu.make_async_copy(*columns(source, index, half, first, count), sems[0])
            for index, source in enumerate((gate_hbm, up_hbm))
            for half in range(2)
        ]
        for c in copies:
            c.start()
        pair = in_pair.at[:, :, pl.ds(2 * first * BLK, 2 * count * BLK)]
        return pltpu.make_async_copy(pair, pair, sems[0]), copies[0]

    bit_loads = []
    for i, (sources, target) in enumerate(
        (
            ((gate_row_hbm, up_row_hbm), in_rows),
            ((gate_col_hbm, up_col_hbm), in_cols),
            ((down_row_hbm,), down_row),
            ((down_col_hbm,), down_col),
            ((order_hbm,), order_out),
        )
    ):
        for j, operand in enumerate(sources):
            into = target if len(sources) == 1 else target.at[j]
            pltpu.make_async_copy(operand, into, bits_sem.at[i]).start()
        bit_loads.append(pltpu.make_async_copy(target, target, bits_sem.at[i]))
    loads = [load(0, 1, (in_sem.at[0], in_sem.at[1]))]
    loads.append(load(1, HBLOCKS - 1, (in_sem.at[2], in_sem.at[3])))

    barrier = pltpu.get_barrier_semaphore()
    links = [(bits[axis], partners[axis][kind]) for axis in range(3) for kind, bits in enumerate(
        ((lax.rem(x, 2), lax.rem(y, 2), z_lo), (lax.div(x, 2), lax.div(y, 2), z_hi))
    )]
    links.append((flip(core), core_partner))
    for is_higher, device in links:

        @pl.when(is_higher == 0)
        def _(device=device):
            pl.semaphore_signal(barrier, inc=1, device_id=device, device_id_type=MESH)

    hadamard = sylvester(2 * BLK)
    plain[...] = hadamard.astype(jnp.bfloat16)
    lower_ends = sum(is_higher for is_higher, _ in links)

    @pl.when(lower_ends > 0)
    def _():
        pl.semaphore_wait(barrier, lower_ends)

    for index, (is_higher, device) in enumerate(links):

        @pl.when(is_higher == 1)
        def _(index=index, device=device):
            pl.semaphore_signal(ready.at[index], inc=1, device_id=device, device_id_type=MESH)

    def mix_in(index, left, chunk):
        for half in range(2):
            if isinstance(chunk, int):
                lanes = pl.ds(half * BLK, BLK)
            else:
                lanes = pl.ds(
                    pl.multiple_of((chunk + 1 + half * (HBLOCKS - 1)) * BLK, BLK), BLK
                )
            bits = in_cols[index, pl.ds(chunk + half * HBLOCKS, 1), :]
            mixed = dot(left[...], in_pair[index, :, lanes]) * signs_of(bits)
            out = pl.ds(half * BLK, BLK)
            own[2 * index, chunk, :, out] = mixed[:BLK]
            own[2 * index + 1, chunk, :, out] = mixed[BLK:]

    def mix_down(chunk):
        first = chunk * BLK
        rows = pl.ds(first if isinstance(chunk, int) else pl.multiple_of(first, BLK), BLK)
        left = plain[:BLK, :BLK].astype(jnp.float32) * signs_of(down_row[pl.ds(chunk, 1), :])
        mixed = dot(left.astype(jnp.bfloat16), down_in[rows, :]) * signs_of(down_col[...])
        own[4, chunk] = mixed[:, :256] + mixed[:, 256:]
        own[5, chunk] = mixed[:, :256] - mixed[:, 256:]

    def mix_right(values):
        upper, lower = split(values)
        return dot(upper, plain[...]) + dot(lower, plain[...])

    def send_first(chunk, groups=range(LANES)):
        for group in groups:
            copy(group, 0, chunk).start()

    def send_when_ready(groups):
        for group in groups:

            @pl.when(links[group][0] == 0)
            def _(group=group):
                pl.semaphore_wait(ready.at[group], 1)
                copy(group, 0, 0).start()

    def mix(chunk):
        mix_in(0, gate_left, chunk)
        mix_in(1, up_left, chunk)
        mix_down(chunk)

    def send_to_lower(groups):
        for group in groups:

            @pl.when(links[group][0] == 1)
            def _(group=group):
                copy(group, 0, 0).start()

    bit_loads[2].wait()
    bit_loads[3].wait()
    loads[0][1].wait()
    mix_down(0)
    bit_loads[0].wait()
    bit_loads[1].wait()
    gate_left[...] = (hadamard * signs_of(in_rows[0])).astype(jnp.bfloat16)
    up_left[...] = (hadamard * signs_of(in_rows[1])).astype(jnp.bfloat16)
    send_to_lower((5, 4))
    loads[0][0].wait()
    mix_in(0, gate_left, 0)
    mix_in(1, up_left, 0)
    send_to_lower(range(4))
    send_when_ready((0, 2, 4, 1, 3))
    loads[1][0].wait()
    loads[1][1].wait()
    bit_loads[4].wait()

    def spread(chunk, carry):
        mix(chunk)
        send_first(chunk)
        return carry

    def second(chunk, carry):
        mix(chunk)
        send_first(chunk, range(5))
        return carry

    lax.fori_loop(1, 2, second, 0)
    send_when_ready((5,))
    send_first(1, (5,))

    @pl.when(core == 1)
    def _():
        pl.semaphore_wait(ready.at[LANES], 1)

    lax.fori_loop(2, HBLOCKS, spread, 0)

    def first_half(slot):
        def step(chunk, carry):
            arrive(slot, chunk)
            for group in range(LANES):
                axis = axis_of(group, slot)
                q = low[axis] if group % 2 == 0 else low[axis] * high[axis]
                mine = source(group, slot)[group, chunk]
                theirs = q * got[slot][group, chunk]
                got[slot][group, chunk] = mine + theirs
                spare(slot)[group, chunk] = mine - theirs
                if group > 0:
                    copy(group - 1, slot + 1, chunk).start()
            copy(LANES - 1, slot + 1, chunk).start()
            return carry

        lax.fori_loop(0, HBLOCKS, step, 0)

    def combined(group, slot, chunk, scale):
        axis = axis_of(group, slot)
        fk = low[axis] * high[axis] * scale
        fr = scale if group % 2 == 0 else high[axis] * scale
        return fr * got[slot][group, chunk] + fk * got[slot - 1][group, chunk]

    def second_half(slot):
        with_core = [group for group in range(LANES) if CORE_AFTER[group] == slot]
        others = [group for group in range(LANES) if CORE_AFTER[group] != slot]

        def settle(first, count):
            part = got_core.at[pl.ds(with_core[0], 3), pl.ds(first, count)]
            await_core(slot, part, unit_of(first)).wait_recv()

            def one_chunk(index, carry):
                last = first + index
                ready = None
                for group in with_core:
                    got_core[group, last] = (
                        got_core[group, last] + core_sign * got[slot][group, last]
                    )
                    if ready is not None:
                        ready.start()
                    ready = copy(group, slot + 1, last)
                ready.start()
                return carry

            lax.fori_loop(0, count, one_chunk, 0)

        def step(chunk, carry):
            arrive(slot, chunk)
            ready = None
            for group in with_core + others:
                values = combined(group, slot, chunk, 1.0)
                if RIGHT_AFTER[group] == slot:
                    values = mix_right(values)
                got[slot][group, chunk] = values
                if ready is not None:
                    ready.start()
                if group in with_core:
                    ready = core_copy(group, chunk)
                else:
                    ready = copy(group, slot + 1, chunk)
            ready.start()

            @pl.when(lax.rem(chunk, UNIT) == UNIT - 1)
            def _():
                settle(chunk - (UNIT - 1), UNIT)

            @pl.when(chunk == HBLOCKS - 1)
            def _():
                settle(chunk, 1)

            return carry

        lax.fori_loop(0, HBLOCKS, step, 0)
        await_core(slot, got_core.at[pl.ds(with_core[0], 3)], 0).wait_send()

    def finish(slot):
        def step(chunk, carry):
            arrive(slot, chunk)
            for group in range(LANES):
                values = combined(group, slot, chunk, FACTOR).astype(jnp.bfloat16)
                out = (gate_out, up_out, down_out)[group // 2]
                part = pl.ds((group % 2) * CHUNK[group // 4], CHUNK[group // 4])
                if group < 4:
                    out[chunk, part, :] = values
                else:
                    out[chunk, :, part] = values
            return carry

        lax.fori_loop(0, HBLOCKS, step, 0)
        await_sends(slot)

    for pair in range(3):
        first_half(2 * pair)
        if pair < 2:
            second_half(2 * pair + 1)
        else:
            finish(2 * pair + 1)


def flush(order_ref, gate_mixed, up_mixed, down_mixed, gate_out, up_out, down_out, sem):
    for block in range(HBLOCKS):
        chosen = order_ref[block]
        for index, mixed, out in ((0, gate_mixed, gate_out), (1, up_mixed, up_out)):
            for half in range(2):
                pltpu.make_async_copy(
                    mixed.at[chosen, :, pl.ds(half * BLK, BLK)],
                    out.at[:, pl.ds((half * HBLOCKS + block) * BLK, BLK)],
                    sem.at[index],
                ).start()
        pltpu.make_async_copy(
            down_mixed.at[chosen], down_out.at[pl.ds(block * BLK, BLK)], sem.at[2]
        ).start()
    for index, out in enumerate((gate_out, up_out, down_out)):
        pltpu.make_async_copy(out, out, sem.at[index]).wait()


def on_device(
    gate_weight,
    up_weight,
    down_weight,
    gate_row_bits,
    gate_col_bits,
    up_row_bits,
    up_col_bits,
    down_row_bits,
    down_col_bits,
    block_order,
):
    wide = pltpu.VMEM((LANES, HBLOCKS) + CHUNK, jnp.float32)
    square = pltpu.VMEM((256, 256), jnp.bfloat16)
    hbm = pl.BlockSpec(memory_space=pl.ANY)
    vmem = pl.BlockSpec(memory_space=pltpu.VMEM)
    weights = (gate_weight, up_weight, down_weight)
    bits = (
        gate_row_bits.reshape(1, -1),
        gate_col_bits.reshape(-1, BLK),
        up_row_bits.reshape(1, -1),
        up_col_bits.reshape(-1, BLK),
        down_row_bits.reshape(-1, BLK),
        down_col_bits.reshape(1, -1),
    )
    in_blocks = pltpu.VMEM((HBLOCKS, 256, 256), jnp.bfloat16)
    *mixed, order = pl.pallas_call(
        kernel,
        out_shape=(in_blocks, in_blocks, pltpu.VMEM((HBLOCKS, 128, 512), jnp.bfloat16), pltpu.SMEM((HBLOCKS,), jnp.int32)),
        in_specs=[hbm] * 10,
        out_specs=(vmem,) * 3 + (pl.BlockSpec(memory_space=pltpu.SMEM),),
        scratch_shapes=[wide] * 9
        + [
            pltpu.VMEM((2,) + gate_weight.shape, jnp.bfloat16),
            pltpu.VMEM(down_weight.shape, jnp.bfloat16),
            pltpu.VMEM((2,) + bits[0].shape, jnp.int32),
            pltpu.VMEM((2,) + bits[1].shape, jnp.int32),
            pltpu.VMEM(bits[4].shape, jnp.int32),
            pltpu.VMEM(bits[5].shape, jnp.int32),
        ]
        + [square] * 3
        + [
            pltpu.SemaphoreType.DMA((4,)),
            pltpu.SemaphoreType.DMA((5,)),
            pltpu.SemaphoreType.DMA((2,)),
            pltpu.SemaphoreType.DMA((SLOTS, -(-HBLOCKS // UNIT))),
            pltpu.SemaphoreType.DMA((1,)),
            pltpu.SemaphoreType.DMA((2, -(-HBLOCKS // UNIT))),
            pltpu.SemaphoreType.REGULAR((LANES + 1,)),
        ],
        compiler_params=pltpu.CompilerParams(
            collective_id=0, has_side_effects=True, vmem_limit_bytes=VMEM_LIMIT
        ),
    )(*bits, *weights, block_order)
    return pl.pallas_call(
        flush,
        out_shape=tuple(jax.ShapeDtypeStruct(w.shape, jnp.bfloat16) for w in weights),
        in_specs=[pl.BlockSpec(memory_space=pltpu.SMEM)] + [vmem] * 3,
        out_specs=(hbm,) * 3,
        scratch_shapes=[pltpu.SemaphoreType.DMA((3,))],
    )(pltpu.with_memory_space_constraint(order, pltpu.SMEM), *(pltpu.with_memory_space_constraint(m, pltpu.VMEM) for m in mixed))


def solution(mesh):
    return jax.shard_map(
        on_device,
        mesh=mesh,
        in_specs=(
            P("row", "col"),
            P("row", "col"),
            P("row", "col"),
            P("row"),
            P("col"),
            P("row"),
            P("col"),
            P("row"),
            P("col"),
            P(),
        ),
        out_specs=(P("row", "col"), P("row", "col"), P("row", "col")),
        check_vma=False,
    )
```

```python
import jax
import jax.numpy as jnp
from jax import lax
from jax.experimental import pallas as pl
from jax.experimental.pallas import tpu as pltpu
from jax.sharding import PartitionSpec as P

D = 4096
BLK = 128
GROUPS = 16
HBLOCKS = 7
FACTOR = (D * GROUPS * BLK) ** (-0.5)
MESH = pl.DeviceIdType.MESH
LANES = 6
SLOTS = 6
CHUNK = (128, 256)
UNIT = 3
CORE_AFTER = (1, 1, 1, 3, 3, 3)
RIGHT_AFTER = (3, 3, 3, 1, 1, 1)
VMEM_LIMIT = 55 * 1024 * 1024


def sylvester(order_size):
    rows = lax.broadcasted_iota(jnp.int32, (order_size, order_size), 0)
    both = jnp.bitwise_and(rows, lax.broadcasted_iota(jnp.int32, rows.shape, 1))
    for shift in (4, 2, 1):
        both = jnp.bitwise_xor(both, jnp.right_shift(both, shift))
    return (1 - 2 * jnp.bitwise_and(both, 1)).astype(jnp.float32)


def signs_of(bits):
    return (1 - 2 * bits).astype(jnp.float32)


def split(values):
    high = values.astype(jnp.bfloat16)
    return high, (values - high.astype(jnp.float32)).astype(jnp.bfloat16)


def dot(left, right):
    return jnp.dot(left, right, preferred_element_type=jnp.float32)


def kernel(
    gate_row_hbm,
    gate_col_hbm,
    up_row_hbm,
    up_col_hbm,
    down_row_hbm,
    down_col_hbm,
    gate_hbm,
    up_hbm,
    down_hbm,
    order_hbm,
    gate_out,
    up_out,
    down_out,
    order_out,
    own,
    got0,
    got1,
    got2,
    got3,
    got4,
    got5,
    got_core,
    sent,
    in_pair,
    down_in,
    in_rows,
    in_cols,
    down_row,
    down_col,
    plain,
    gate_left,
    up_left,
    in_sem,
    bits_sem,
    send_sem,
    recv_sem,
    core_send_sem,
    core_recv_sem,
    ready,
):
    got = (got0, got1, got2, got3, got4, got5)
    row, col = lax.axis_index("row"), lax.axis_index("col")
    core = lax.rem(row, 2)
    x = lax.rem(lax.div(row, 2), 4)
    z_lo = lax.div(row, 8)
    y = lax.rem(col, 4)
    z_hi = lax.div(col, 4)

    def flip(bit):
        return 1 - bit

    def place(z_lo, x, core, z_hi, y):
        return (z_lo * 8 + x * 2 + core, z_hi * 4 + y)

    def one(v):
        return v + 1 - 2 * lax.rem(v, 2)

    partners = (
        (place(z_lo, one(x), core, z_hi, y), place(z_lo, 3 - x, core, z_hi, y)),
        (place(z_lo, x, core, z_hi, one(y)), place(z_lo, x, core, z_hi, 3 - y)),
        (place(flip(z_lo), x, core, z_hi, y), place(flip(z_lo), x, core, flip(z_hi), y)),
    )
    core_partner = place(z_lo, x, flip(core), z_hi, y)

    def as_sign(bit):
        return (1 - 2 * bit).astype(jnp.float32)

    low = (as_sign(lax.rem(x, 2)), as_sign(lax.rem(y, 2)), as_sign(z_lo))
    high = (as_sign(lax.div(x, 2)), as_sign(lax.div(y, 2)), as_sign(z_hi))
    core_sign = as_sign(core)

    def axis_of(group, slot):
        return (group // 2 + slot // 2) % 3

    def partner(group, slot):
        return partners[axis_of(group, slot)][(slot + group) % 2]

    def spare(slot):
        return got[slot - 2] if slot else sent

    def source(group, slot):
        if slot == 0:
            return own
        if slot % 2 == 1:
            return spare(slot - 1)
        return got_core if CORE_AFTER[group] == slot - 1 else got[slot - 1]

    def unit_of(chunk):
        return chunk // UNIT if isinstance(chunk, int) else lax.div(chunk, UNIT)

    def copy(group, slot, chunk):
        return pltpu.make_async_remote_copy(
            src_ref=source(group, slot).at[group, chunk],
            dst_ref=got[slot].at[group, chunk],
            send_sem=send_sem.at[slot % 2],
            recv_sem=recv_sem.at[slot, unit_of(chunk)],
            device_id=partner(group, slot),
            device_id_type=MESH,
        )

    def await_chunks(slot, chunk, count):
        part = got[slot].at[:, pl.ds(chunk, count)]
        pltpu.make_async_remote_copy(
            src_ref=part,
            dst_ref=part,
            send_sem=send_sem.at[slot % 2],
            recv_sem=recv_sem.at[slot, unit_of(chunk)],
            device_id=core_partner,
            device_id_type=MESH,
        ).wait_recv()

    def await_sends(slot):
        pltpu.make_async_remote_copy(
            src_ref=got[slot],
            dst_ref=got[slot],
            send_sem=send_sem.at[slot % 2],
            recv_sem=recv_sem.at[slot, 0],
            device_id=core_partner,
            device_id_type=MESH,
        ).wait_send()

    def arrive(slot, chunk):
        @pl.when((lax.rem(chunk, UNIT) == 0) & (chunk < HBLOCKS - 1))
        def _():
            await_chunks(slot, chunk, UNIT)

        @pl.when(chunk == HBLOCKS - 1)
        def _():
            await_chunks(slot, chunk, 1)

        if slot > 0:

            @pl.when(chunk == 0)
            def _():
                await_sends(slot - 1)

    def core_copy(group, chunk):
        return pltpu.make_async_remote_copy(
            src_ref=got[CORE_AFTER[group]].at[group, chunk],
            dst_ref=got_core.at[group, chunk],
            send_sem=core_send_sem.at[0],
            recv_sem=core_recv_sem.at[group // 3, unit_of(chunk)],
            device_id=core_partner,
            device_id_type=MESH,
        )

    def await_core(slot, part, recv_unit):
        every = pltpu.make_async_remote_copy(
            src_ref=part,
            dst_ref=part,
            send_sem=core_send_sem.at[0],
            recv_sem=core_recv_sem.at[slot // 2, recv_unit],
            device_id=core_partner,
            device_id_type=MESH,
        )
        return every

    def columns(source, index, half, first, count):
        lanes = pl.ds((half * HBLOCKS + first) * BLK, count * BLK)
        into = pl.ds((first * 2 + half * count) * BLK, count * BLK)
        return source.at[:, lanes], in_pair.at[index, :, into]

    def load(first, count, sems):
        rows = pl.ds(first * BLK, count * BLK)
        copies = [pltpu.make_async_copy(down_hbm.at[rows], down_in.at[rows], sems[1])]
        copies += [
            pltpu.make_async_copy(*columns(source, index, half, first, count), sems[0])
            for index, source in enumerate((gate_hbm, up_hbm))
            for half in range(2)
        ]
        for c in copies:
            c.start()
        pair = in_pair.at[:, :, pl.ds(2 * first * BLK, 2 * count * BLK)]
        return pltpu.make_async_copy(pair, pair, sems[0]), copies[0]

    bit_loads = []
    for i, (sources, target) in enumerate(
        (
            ((gate_row_hbm, up_row_hbm), in_rows),
            ((gate_col_hbm, up_col_hbm), in_cols),
            ((down_row_hbm,), down_row),
            ((down_col_hbm,), down_col),
            ((order_hbm,), order_out),
        )
    ):
        for j, operand in enumerate(sources):
            into = target if len(sources) == 1 else target.at[j]
            pltpu.make_async_copy(operand, into, bits_sem.at[i]).start()
        bit_loads.append(pltpu.make_async_copy(target, target, bits_sem.at[i]))
    loads = [load(0, 1, (in_sem.at[0], in_sem.at[1]))]
    loads.append(load(1, HBLOCKS - 1, (in_sem.at[2], in_sem.at[3])))

    barrier = pltpu.get_barrier_semaphore()
    links = [(bits[axis], partners[axis][kind]) for axis in range(3) for kind, bits in enumerate(
        ((lax.rem(x, 2), lax.rem(y, 2), z_lo), (lax.div(x, 2), lax.div(y, 2), z_hi))
    )]
    links.append((flip(core), core_partner))
    for is_higher, device in links:

        @pl.when(is_higher == 0)
        def _(device=device):
            pl.semaphore_signal(barrier, inc=1, device_id=device, device_id_type=MESH)

    lower_ends = sum(is_higher for is_higher, _ in links)

    @pl.when(lower_ends > 0)
    def _():
        pl.semaphore_wait(barrier, lower_ends)

    for index, (is_higher, device) in enumerate(links):

        @pl.when(is_higher == 1)
        def _(index=index, device=device):
            pl.semaphore_signal(ready.at[index], inc=1, device_id=device, device_id_type=MESH)

    hadamard = sylvester(2 * BLK)
    plain[...] = hadamard.astype(jnp.bfloat16)
    def mix_in(index, left, chunk):
        for half in range(2):
            if isinstance(chunk, int):
                lanes = pl.ds(half * BLK, BLK)
            else:
                lanes = pl.ds(
                    pl.multiple_of((chunk + 1 + half * (HBLOCKS - 1)) * BLK, BLK), BLK
                )
            bits = in_cols[index, pl.ds(chunk + half * HBLOCKS, 1), :]
            mixed = dot(left[...], in_pair[index, :, lanes]) * signs_of(bits)
            out = pl.ds(half * BLK, BLK)
            own[2 * index, chunk, :, out] = mixed[:BLK]
            own[2 * index + 1, chunk, :, out] = mixed[BLK:]

    def mix_down(chunk):
        first = chunk * BLK
        rows = pl.ds(first if isinstance(chunk, int) else pl.multiple_of(first, BLK), BLK)
        left = plain[:BLK, :BLK].astype(jnp.float32) * signs_of(down_row[pl.ds(chunk, 1), :])
        mixed = dot(left.astype(jnp.bfloat16), down_in[rows, :]) * signs_of(down_col[...])
        own[4, chunk] = mixed[:, :256] + mixed[:, 256:]
        own[5, chunk] = mixed[:, :256] - mixed[:, 256:]

    def mix_right(values):
        upper, lower = split(values)
        return dot(upper, plain[...]) + dot(lower, plain[...])

    def send_first(chunk, groups=range(LANES)):
        for group in groups:
            copy(group, 0, chunk).start()

    def send_when_ready(groups):
        for group in groups:

            @pl.when(links[group][0] == 0)
            def _(group=group):
                pl.semaphore_wait(ready.at[group], 1)
                copy(group, 0, 0).start()

    def mix(chunk):
        mix_in(0, gate_left, chunk)
        mix_in(1, up_left, chunk)
        mix_down(chunk)

    def send_to_lower(groups):
        for group in groups:

            @pl.when(links[group][0] == 1)
            def _(group=group):
                copy(group, 0, 0).start()

    bit_loads[2].wait()
    bit_loads[3].wait()
    loads[0][1].wait()
    mix_down(0)
    bit_loads[0].wait()
    bit_loads[1].wait()
    gate_left[...] = (hadamard * signs_of(in_rows[0])).astype(jnp.bfloat16)
    up_left[...] = (hadamard * signs_of(in_rows[1])).astype(jnp.bfloat16)
    send_to_lower((5, 4))
    loads[0][0].wait()
    mix_in(0, gate_left, 0)
    mix_in(1, up_left, 0)
    send_to_lower(range(4))
    send_when_ready((0, 2, 4, 1, 3))
    loads[1][0].wait()
    loads[1][1].wait()
    bit_loads[4].wait()

    def spread(chunk, carry):
        mix(chunk)
        send_first(chunk)
        return carry

    def second(chunk, carry):
        mix(chunk)
        send_first(chunk, range(5))
        return carry

    lax.fori_loop(1, 2, second, 0)
    send_when_ready((5,))
    send_first(1, (5,))

    @pl.when(core == 1)
    def _():
        pl.semaphore_wait(ready.at[LANES], 1)

    lax.fori_loop(2, HBLOCKS, spread, 0)

    def first_half(slot):
        def step(chunk, carry):
            arrive(slot, chunk)
            for group in range(LANES):
                axis = axis_of(group, slot)
                q = low[axis] if group % 2 == 0 else low[axis] * high[axis]
                mine = source(group, slot)[group, chunk]
                theirs = q * got[slot][group, chunk]
                got[slot][group, chunk] = mine + theirs
                spare(slot)[group, chunk] = mine - theirs
                if group > 0:
                    copy(group - 1, slot + 1, chunk).start()
            copy(LANES - 1, slot + 1, chunk).start()
            return carry

        lax.fori_loop(0, HBLOCKS, step, 0)

    def combined(group, slot, chunk, scale):
        axis = axis_of(group, slot)
        fk = low[axis] * high[axis] * scale
        fr = scale if group % 2 == 0 else high[axis] * scale
        return fr * got[slot][group, chunk] + fk * got[slot - 1][group, chunk]

    def second_half(slot):
        with_core = [group for group in range(LANES) if CORE_AFTER[group] == slot]
        others = [group for group in range(LANES) if CORE_AFTER[group] != slot]

        def settle(first, count):
            part = got_core.at[pl.ds(with_core[0], 3), pl.ds(first, count)]
            await_core(slot, part, unit_of(first)).wait_recv()

            def one_chunk(index, carry):
                last = first + index
                ready = None
                for group in with_core:
                    got_core[group, last] = (
                        got_core[group, last] + core_sign * got[slot][group, last]
                    )
                    if ready is not None:
                        ready.start()
                    ready = copy(group, slot + 1, last)
                ready.start()
                return carry

            lax.fori_loop(0, count, one_chunk, 0)

        def step(chunk, carry):
            arrive(slot, chunk)
            ready = None
            for group in with_core + others:
                values = combined(group, slot, chunk, 1.0)
                if RIGHT_AFTER[group] == slot:
                    values = mix_right(values)
                got[slot][group, chunk] = values
                if ready is not None:
                    ready.start()
                if group in with_core:
                    ready = core_copy(group, chunk)
                else:
                    ready = copy(group, slot + 1, chunk)
            ready.start()

            @pl.when(lax.rem(chunk, UNIT) == UNIT - 1)
            def _():
                settle(chunk - (UNIT - 1), UNIT)

            @pl.when(chunk == HBLOCKS - 1)
            def _():
                settle(chunk, 1)

            return carry

        lax.fori_loop(0, HBLOCKS, step, 0)
        await_core(slot, got_core.at[pl.ds(with_core[0], 3)], 0).wait_send()

    def finish(slot):
        def step(chunk, carry):
            arrive(slot, chunk)
            for group in range(LANES):
                values = combined(group, slot, chunk, FACTOR).astype(jnp.bfloat16)
                out = (gate_out, up_out, down_out)[group // 2]
                part = pl.ds((group % 2) * CHUNK[group // 4], CHUNK[group // 4])
                if group < 4:
                    out[chunk, part, :] = values
                else:
                    out[chunk, :, part] = values
            return carry

        lax.fori_loop(0, HBLOCKS, step, 0)
        await_sends(slot)

    for pair in range(3):
        first_half(2 * pair)
        if pair < 2:
            second_half(2 * pair + 1)
        else:
            finish(2 * pair + 1)


def flush(order_ref, gate_mixed, up_mixed, down_mixed, gate_out, up_out, down_out, sem):
    for block in range(HBLOCKS):
        chosen = order_ref[block]
        for index, mixed, out in ((0, gate_mixed, gate_out), (1, up_mixed, up_out)):
            for half in range(2):
                pltpu.make_async_copy(
                    mixed.at[chosen, :, pl.ds(half * BLK, BLK)],
                    out.at[:, pl.ds((half * HBLOCKS + block) * BLK, BLK)],
                    sem.at[index],
                ).start()
        pltpu.make_async_copy(
            down_mixed.at[chosen], down_out.at[pl.ds(block * BLK, BLK)], sem.at[2]
        ).start()
    for index, out in enumerate((gate_out, up_out, down_out)):
        pltpu.make_async_copy(out, out, sem.at[index]).wait()


def on_device(
    gate_weight,
    up_weight,
    down_weight,
    gate_row_bits,
    gate_col_bits,
    up_row_bits,
    up_col_bits,
    down_row_bits,
    down_col_bits,
    block_order,
):
    wide = pltpu.VMEM((LANES, HBLOCKS) + CHUNK, jnp.float32)
    square = pltpu.VMEM((256, 256), jnp.bfloat16)
    hbm = pl.BlockSpec(memory_space=pl.ANY)
    vmem = pl.BlockSpec(memory_space=pltpu.VMEM)
    weights = (gate_weight, up_weight, down_weight)
    bits = (
        gate_row_bits.reshape(1, -1),
        gate_col_bits.reshape(-1, BLK),
        up_row_bits.reshape(1, -1),
        up_col_bits.reshape(-1, BLK),
        down_row_bits.reshape(-1, BLK),
        down_col_bits.reshape(1, -1),
    )
    in_blocks = pltpu.VMEM((HBLOCKS, 256, 256), jnp.bfloat16)
    *mixed, order = pl.pallas_call(
        kernel,
        out_shape=(in_blocks, in_blocks, pltpu.VMEM((HBLOCKS, 128, 512), jnp.bfloat16), pltpu.SMEM((HBLOCKS,), jnp.int32)),
        in_specs=[hbm] * 10,
        out_specs=(vmem,) * 3 + (pl.BlockSpec(memory_space=pltpu.SMEM),),
        scratch_shapes=[wide] * 9
        + [
            pltpu.VMEM((2,) + gate_weight.shape, jnp.bfloat16),
            pltpu.VMEM(down_weight.shape, jnp.bfloat16),
            pltpu.VMEM((2,) + bits[0].shape, jnp.int32),
            pltpu.VMEM((2,) + bits[1].shape, jnp.int32),
            pltpu.VMEM(bits[4].shape, jnp.int32),
            pltpu.VMEM(bits[5].shape, jnp.int32),
        ]
        + [square] * 3
        + [
            pltpu.SemaphoreType.DMA((4,)),
            pltpu.SemaphoreType.DMA((5,)),
            pltpu.SemaphoreType.DMA((2,)),
            pltpu.SemaphoreType.DMA((SLOTS, -(-HBLOCKS // UNIT))),
            pltpu.SemaphoreType.DMA((1,)),
            pltpu.SemaphoreType.DMA((2, -(-HBLOCKS // UNIT))),
            pltpu.SemaphoreType.REGULAR((LANES + 1,)),
        ],
        compiler_params=pltpu.CompilerParams(
            collective_id=0, has_side_effects=True, vmem_limit_bytes=VMEM_LIMIT
        ),
    )(*bits, *weights, block_order)
    return pl.pallas_call(
        flush,
        out_shape=tuple(jax.ShapeDtypeStruct(w.shape, jnp.bfloat16) for w in weights),
        in_specs=[pl.BlockSpec(memory_space=pltpu.SMEM)] + [vmem] * 3,
        out_specs=(hbm,) * 3,
        scratch_shapes=[pltpu.SemaphoreType.DMA((3,))],
    )(pltpu.with_memory_space_constraint(order, pltpu.SMEM), *(pltpu.with_memory_space_constraint(m, pltpu.VMEM) for m in mixed))


def solution(mesh):
    return jax.shard_map(
        on_device,
        mesh=mesh,
        in_specs=(
            P("row", "col"),
            P("row", "col"),
            P("row", "col"),
            P("row"),
            P("col"),
            P("row"),
            P("col"),
            P("row"),
            P("col"),
            P(),
        ),
        out_specs=(P("row", "col"), P("row", "col"), P("row", "col")),
        check_vma=False,
    )
```
